32 devices in a mesh: row: 2 (over y), col: 8 (over z, x), layer: 2 (over core).
Axes of the slice: x: 2, y: 2, z: 4, core: 2. Of those that a mesh axis runs over, the one named last changes fastest.
Arguments:
- anomaly_x: bfloat16 [8, 4096, 4096], P(None, 'row', ('layer', 'col')), may hold values from -0.09375 to 0.09375
- anomaly_y: bfloat16 [8, 4096, 4096], P(None, 'col', ('layer', 'row')), may hold values from -6 to 6
Outputs:
- covariance: bfloat16 [8, 4096, 4096], P('layer', 'row', 'col')
The draws below stay inside these ranges and needn't reach their ends.
All inputs are finite; a program needn't handle non-finite values.
Results may differ from the reference program's by a relative error of at most 0.001.
Values may be sent and summed in bfloat16 or wider, within the bound.
A program may use at most 192 MiB of HBM per device.

```python
import jax
import jax.numpy as jnp
from jax import lax

BATCH = 8
NSTATE = 4096
MEMBERS = 4096


def raised(values, own_key, source, target, shards_of, factor):
    owner, partner = [(jnp.arange(values.shape[axis_at]) // (values.shape[axis_at] // shards_of)).reshape([-1 if axis == axis_at else 1 for axis in range(values.ndim)]) for axis_at in (source, target)]
    chosen = jax.random.permutation(own_key, shards_of)[partner]
    strong = (owner == chosen) | (owner == (partner + shards_of // 2) % shards_of)
    return jnp.where(strong, factor * values, values)


def steps_of(rng, dims, cuts, least, top_value):
    level, own = 1.0, jax.random.fold_in(rng, 6)
    for position, shards_of in cuts:
        steps = jnp.exp(jax.random.uniform(jax.random.fold_in(own, position), (shards_of,), jnp.float32, least / len(cuts), top_value / len(cuts)))
        level = level * jnp.repeat(steps, dims[position] // shards_of).reshape([-1 if axis == position else 1 for axis in range(len(dims))])
    return level


def noise(rng, shape, deviation, reach, pieces=(), held_as=jnp.bfloat16):
    gain = steps_of(rng, shape, pieces, -0.22, 0.18) if pieces else 1.0
    drawn = jax.random.normal(rng, shape, jnp.float32) * deviation * gain
    return jnp.minimum(jnp.maximum(drawn, -reach), reach).astype(held_as)


def heavy_noise(stream_key, dims, deviation, reach, shards, heavy, kind=jnp.bfloat16):
    result = deviation * jax.random.normal(stream_key, dims, jnp.float32)
    if shards:
        result = result * steps_of(stream_key, dims, shards, -0.22, 0.18)
    return jnp.clip(raised(result, jax.random.fold_in(stream_key, 3), *heavy), -reach, reach).astype(kind)


def setup_inputs(seed: int = 0) -> dict:
    key_of = jax.random.split(jax.random.key(seed), 3)
    return {
        "anomaly_x": noise(key_of[0], (BATCH, NSTATE, MEMBERS), MEMBERS ** -0.5, 0.09375, ((1, 2), (2, 16))),
        "anomaly_y": heavy_noise(key_of[1], (BATCH, NSTATE, MEMBERS), 1.0, 6.0, ((1, 8), (2, 4)), (2, 0, 4, 2.0)),
    }


def one_product(pair):
    left, right = pair
    return jnp.dot(left, right.T, preferred_element_type=jnp.float32).astype(jnp.bfloat16)


def reference(anomaly_x, anomaly_y):
    return lax.map(one_product, (anomaly_x, anomaly_y))
```

```python
import functools

import jax
import jax.numpy as jnp
from jax import lax
from jax.experimental import pallas as pl
from jax.experimental.pallas import tpu as pltpu
from jax.sharding import PartitionSpec as P

LANES = 128
MESH = pl.DeviceIdType.MESH
NT = (((1,), (1,)), ((), ()))


def gathered(anomaly_x, anomaly_y):
    panel_x = lax.all_gather(anomaly_x, "col", axis=2, tiled=True)
    partial_tile = jnp.einsum(
        "bik,bjk->bij",
        panel_x,
        lax.all_gather(anomaly_y, "row", axis=2, tiled=True),
        preferred_element_type=jnp.float32,
    )
    summed = lax.psum_scatter(partial_tile, "layer", scatter_dimension=0, tiled=True)
    return summed.astype(jnp.bfloat16)


def plan():
    recv = {}

    def add(*key):
        recv[key] = len(recv)

    for rel in range(4):
        for ec in range(2):
            for ex in range(2):
                if rel or ec or ex:
                    add("x0", rel, ec, ex)
    for ec in range(2):
        for ex in range(2):
            if ec or ex:
                add("x1", ec, ex)
            for yr in range(2):
                if ec or ex or yr:
                    add("y0", ec, ex, yr)
                    add("y1", 0, ec, ex, yr)
                add("y1", 1, ec, ex, yr)
    for kind in ("out0", "out1", "out2"):
        add(kind)
    return recv


RECV = plan()
SENDS = 48


def kernel(
    sizes, x_ref, y_ref, o_ref, xg, yg0, yg1, og0, og1,
    local_sem, send_sem, recv_sem, up_send, up_recv, near_send, far_send, near_recv, far_recv,
    o0_send, o0_keep, o1_send, o1_keep,
):
    rows, planes, lines, layers = sizes
    y, col, c = lax.axis_index("row"), lax.axis_index("col"), lax.axis_index("layer")
    z, x = col // lines, lax.rem(col, lines)
    depth_x, depth_y = x_ref.shape[2], y_ref.shape[2]
    height, width = x_ref.shape[1], y_ref.shape[1]
    group = depth_x * planes * lines
    pair = depth_x * lines
    chunk = og0.shape[1]
    count = height // chunk
    slots0, slots1 = og0.shape[0], og1.shape[0]

    half = z // 2
    mid, end = 1 + half, 3 * half
    inner = (z == 1) | (z == 2)
    partner = z + 1 - 2 * lax.rem(z, 2)
    across = planes - 1 - z
    level = [z, partner, planes - 1 - mid, planes - 1 - end]

    def core(e):
        return lax.rem(c + e, layers)

    def line(e):
        return lax.rem(x + e, lines)

    def row(e):
        return lax.rem(y + e, rows)

    def dev(yy, zz, xx, cc):
        return {"row": yy, "col": zz * lines + xx, "layer": cc}

    def batch(ec, ex, s):
        return core(ec) * planes + line(ex) * 2 + s

    def xcols(rel, ec, ex):
        return pl.ds(pl.multiple_of(core(ec) * group + (level[rel] * lines + line(ex)) * depth_x, depth_x), depth_x)

    def xpair(rel, ec):
        return pl.ds(pl.multiple_of(core(ec) * group + level[rel] * pair, pair), pair)

    def ycols(ec, er):
        return pl.ds(pl.multiple_of(core(ec) * group + row(er) * depth_y, depth_y), depth_y)

    def y0zone(ec, ex, er):
        return yg0.at[pl.ds(pl.multiple_of(line(ex) * width, width), width), ycols(ec, er)]

    def y1zone(rel, ec, ex, er):
        at = lax.rem(level[rel], 2) * lines * width + line(ex) * width
        return yg1.at[pl.ds(pl.multiple_of(at, width), width), ycols(ec, er)]

    def rowsof(r):
        return pl.ds(pl.multiple_of(r * chunk, chunk), chunk)

    def tile(q):
        return pl.ds(pl.multiple_of(q * width, width), width)

    peers = [dev(y, z, line(ex), core(ec)) for ec in range(2) for ex in range(2) if ec or ex]
    peers += [dev(row(1), z, x, c), dev(y, partner, x, c), dev(y, partner, line(1), c), dev(y, across, x, c)]
    barrier = pltpu.get_barrier_semaphore()
    for peer in peers:
        pl.semaphore_signal(barrier, inc=1, device_id=peer, device_id_type=MESH)
    pl.semaphore_wait(barrier, len(peers))

    over_y, over_half, over_mid = dev(row(1), z, x, c), dev(y, partner, x, c), dev(y, across, x, c)

    def remote(src, dst, s, r, to):
        return pltpu.make_async_remote_copy(
            src_ref=src, dst_ref=dst, send_sem=s, recv_sem=r, device_id=to, device_id_type=MESH
        )

    def landed(dst, sem):
        remote(dst, dst, sem, sem, over_y).wait_recv()

    sent = []

    def push(log, src, dst, key, to):
        cp = remote(src, dst, send_sem.at[len(log)], recv_sem.at[RECV[key]], to)
        cp.start()
        log.append(cp)

    def await_x0(rel, ec, ex):
        landed(xg.at[0, :, xcols(rel, ec, ex)], recv_sem.at[RECV["x0", rel, ec, ex]])

    def await_x1(ec, ex):
        landed(xg.at[1, :, xcols(0, ec, ex)], recv_sem.at[RECV["x1", ec, ex]])

    def await_y0(ec, ex, er):
        landed(y0zone(ec, ex, er), recv_sem.at[RECV["y0", ec, ex, er]])

    def await_y1(rel, ec, ex, er):
        landed(y1zone(rel, ec, ex, er), recv_sem.at[RECV["y1", rel, ec, ex, er]])

    def send_x0(log, rel, ec, ex, to, there):
        zone = xg.at[0, :, xcols(rel, ec, ex)]
        src = zone if rel or ec or ex else x_ref.at[batch(0, 0, 0)]
        push(log, src, zone, ("x0", there, ec, ex), to)

    def send_y0(log, ec, ex):
        zone = y0zone(ec, ex, 0)
        src = zone if ec or ex else y_ref.at[batch(0, 0, 0)]
        push(log, src, zone, ("y0", ec, ex, 1), over_y)

    def send_y1(log, rel, ec, ex, to, there, er):
        zone = y1zone(rel, ec, ex, 0)
        src = zone if rel or ec or ex else y_ref.at[batch(0, 0, 1)]
        push(log, src, zone, ("y1", there, ec, ex, er), to)

    def spread(ec, ex):
        to = dev(y, z, line(ex), core(ec))
        own = (0, 0)
        push(sent, x_ref.at[batch(ec, ex, 0)], xg.at[0, :, xcols(0, *own)], ("x0", 0, ec, ex), to)
        push(sent, y_ref.at[batch(ec, ex, 1)], y1zone(0, *own, 0), ("y1", 0, ec, ex, 0), to)
        push(sent, x_ref.at[batch(ec, ex, 1)], xg.at[1, :, xcols(0, *own)], ("x1", ec, ex), to)
        push(sent, y_ref.at[batch(ec, ex, 0)], y0zone(*own, 0), ("y0", ec, ex, 0), to)

    def spread_line():
        own = (0, 0)
        for what in range(4):
            for ec in range(2):
                to = dev(y, z, line(1), core(ec))
                if what == 0:
                    push(sent, x_ref.at[batch(ec, 1, 0)], xg.at[0, :, xcols(0, *own)], ("x0", 0, ec, 1), to)
                elif what == 1:
                    push(sent, y_ref.at[batch(ec, 1, 1)], y1zone(0, *own, 0), ("y1", 0, ec, 1, 0), to)
                elif what == 2:
                    push(sent, x_ref.at[batch(ec, 1, 1)], xg.at[1, :, xcols(0, *own)], ("x1", ec, 1), to)
                else:
                    push(sent, y_ref.at[batch(ec, 1, 0)], y0zone(*own, 0), ("y0", ec, 1, 0), to)

    send_x0(sent, 0, 0, 0, over_half, 1)
    spread(1, 0)
    spread_line()
    keeps = [
        pltpu.make_async_copy(x_ref.at[batch(0, 0, s)], xg.at[s, :, xcols(0, 0, 0)], local_sem.at[s]) for s in range(2)
    ] + [
        pltpu.make_async_copy(y_ref.at[batch(0, 0, 0)], y0zone(0, 0, 0), local_sem.at[2]),
        pltpu.make_async_copy(y_ref.at[batch(0, 0, 1)], y1zone(0, 0, 0, 0), local_sem.at[3]),
    ]
    for keep in keeps:
        keep.start()

    def out0(k, e):
        slot = lax.rem(k, slots0)
        src = og0.at[slot, :, tile(line(e))]
        dst = o_ref.at[x * 2, rowsof(k)]
        if e == 0:
            return pltpu.make_async_copy(src, dst, o0_keep.at[slot])
        return remote(src, dst, o0_send.at[slot], recv_sem.at[RECV[("out0",)]], dev(y, z, line(1), c))

    def free0(k):
        out0(k, 0).wait()
        out0(k, 1).wait_send()

    def product0(k):
        pl.when(k >= slots0)(lambda: free0(k - slots0))
        og0[lax.rem(k, slots0)] = lax.dot_general(
            xg[0, rowsof(k), :], yg0[...], NT, preferred_element_type=jnp.float32
        ).astype(jnp.bfloat16)
        out0(k, 0).start()
        out0(k, 1).start()

    def out1(r, ez, ex):
        slot = lax.rem(r, slots1)
        zz = lax.rem(level[ez], 2)
        src = og1.at[slot, :, tile(zz * lines + line(ex))]
        dst = o_ref.at[x * 2 + 1, rowsof(r)]
        if not ez and not ex:
            return pltpu.make_async_copy(src, dst, o1_keep.at[slot])
        kind = "out1" if ez == 0 or ex == 0 else "out2"
        return remote(src, dst, o1_send.at[slot * 3 + ez * 2 + ex - 1], recv_sem.at[RECV[(kind,)]],
                      dev(y, level[ez], line(ex), c))

    def free1(r):
        out1(r, 0, 0).wait()
        for ez, ex in ((1, 1), (1, 0), (0, 1)):
            out1(r, ez, ex).wait_send()

    def near(r, ec, to, sems):
        zone = xg.at[1, rowsof(r), xpair(0, ec)]
        return remote(zone, zone, near_send.at[r * 2 + ec], sems.at[r * 2 + ec], to)

    def far(r, ec):
        zone = xg.at[1, rowsof(r), xpair(1, ec)]
        return remote(zone, zone, far_send.at[r * 2 + ec], far_recv.at[r * 2 + ec], over_mid)

    def send_near(r):
        for ec in range(2):
            near(r, ec, over_mid, near_recv).start()

    def send_far(r):
        for ec in range(2):
            landed(xg.at[1, rowsof(r), xpair(1, ec)], up_recv.at[r * 2 + ec])
            far(r, ec).start()

    def product1(r):
        for ec in range(2):
            landed(xg.at[1, rowsof(r), xpair(2, ec)], near_recv.at[r * 2 + ec])
            landed(xg.at[1, rowsof(r), xpair(3, ec)], far_recv.at[r * 2 + ec])
        pl.when(r >= slots1)(lambda: free1(r - slots1))
        slot, wide = lax.rem(r, slots1), lines * width

        def part(q, _):
            at = pl.ds(pl.multiple_of(q * wide, wide), wide)
            og1[slot, :, at] = lax.dot_general(
                xg[1, rowsof(r), :], yg1[at, :], NT, preferred_element_type=jnp.float32
            ).astype(jnp.bfloat16)
            return 0

        lax.fori_loop(0, 2, part, 0)
        for ez, ex in ((1, 1), (1, 0), (0, 1), (0, 0)):
            out1(r, ez, ex).start()

    ahead = 4

    @pl.when(inner)
    def _():
        log = list(sent)
        send_x0(log, 0, 0, 0, over_mid, 2)
        send_y1(log, 0, 0, 0, over_y, 0, 1)

        def own(ec, ex):
            await_x0(0, ec, ex)
            send_x0(log, 0, ec, ex, over_mid, 2)
            send_x0(log, 0, ec, ex, over_half, 1)

        def outer(ec, ex):
            await_x0(1, ec, ex)
            send_x0(log, 1, ec, ex, over_mid, 3)

        def other(rel, ec, ex):
            await_x0(rel, ec, ex)
            send_x0(log, rel, ec, ex, over_half, rel)

        def side0(ec, ex):
            await_y0(ec, ex, 0)
            send_y0(log, ec, ex)

        def side1(rel, ec, ex):
            await_y1(rel, ec, ex, 0)
            send_y1(log, rel, ec, ex, over_y, rel, 1)

        own(1, 0)
        side1(0, 1, 0)
        send_y0(log, 0, 0)
        own(0, 1)
        outer(0, 0)
        other(2, 0, 0)
        own(1, 1)
        outer(1, 0)
        other(2, 1, 0)
        side1(0, 0, 1)
        other(2, 0, 1)
        side1(1, 0, 0)
        side1(0, 1, 1)
        side1(1, 1, 0)
        side0(1, 0)
        other(2, 1, 1)
        outer(0, 1)
        other(3, 0, 0)
        outer(1, 1)
        other(3, 1, 0)
        keeps[1].wait()
        await_x1(1, 0)
        await_x1(0, 1)
        await_x1(1, 1)
        send_near(0)
        send_near(1)
        side1(1, 0, 1)
        other(3, 0, 1)
        side0(0, 1)
        side1(1, 1, 1)
        other(3, 1, 1)
        side0(1, 1)
        for r in range(ahead):
            send_far(r)
            send_near(r + 2)
        keeps[0].wait()
        keeps[2].wait()
        keeps[3].wait()
        for rel in range(2):
            for ec in range(2):
                for ex in range(2):
                    await_y1(rel, ec, ex, 1)

        def both(r, _):
            product1(r)

            @pl.when(r + ahead < count)
            def _():
                send_far(r + ahead)

            @pl.when(r + ahead + 2 < count)
            def _():
                send_near(r + ahead + 2)

            @pl.when(r == 3)
            def _():
                for ec in range(2):
                    for ex in range(2):
                        await_y0(ec, ex, 1)

            @pl.when((r >= 3) & (r < 7))
            def _():
                def step(k, _):
                    product0((r - 3) * (count // 4) + k)
                    return 0

                lax.fori_loop(0, count // 4, step, 0)

            return 0

        lax.fori_loop(0, count, both, 0)
        for r in range(count):
            for ec in range(2):
                near(r, ec, over_mid, near_recv).wait_send()
                far(r, ec).wait_send()
        for r in range(count - slots1, count):
            free1(r)
        for k in range(count - slots0, count):
            free0(k)
        landed(o_ref.at[line(1) * 2], recv_sem.at[RECV[("out0",)]])
        landed(o_ref.at[line(1) * 2 + 1], recv_sem.at[RECV[("out1",)]])
        for cp in log:
            cp.wait_send()

    @pl.when(jnp.logical_not(inner))
    def _():
        log = list(sent)

        def own(ec, ex):
            await_x0(0, ec, ex)
            send_x0(log, 0, ec, ex, over_half, 1)

        def side0(ec, ex):
            await_y0(ec, ex, 0)
            send_y0(log, ec, ex)

        def down(ec, ex):
            if ec or ex:
                await_y1(0, ec, ex, 0)
            send_y1(log, 0, ec, ex, over_half, 1, 0)

        own(1, 0)
        down(0, 0)
        down(1, 0)
        send_y0(log, 0, 0)
        side0(1, 0)
        own(0, 1)
        own(1, 1)
        down(0, 1)
        down(1, 1)
        keeps[1].wait()
        await_x1(1, 0)
        await_x1(0, 1)
        await_x1(1, 1)
        for r in range(count):
            for ec in range(2):
                near(r, ec, over_half, up_recv).start()
        side0(0, 1)
        side0(1, 1)
        keeps[0].wait()
        keeps[2].wait()
        keeps[3].wait()
        for ec in range(2):
            for ex in range(2):
                await_y0(ec, ex, 1)
        for rel in range(1, 4):
            for ec in range(2):
                for ex in range(2):
                    await_x0(rel, ec, ex)

        def step(k, _):
            product0(k)
            return 0

        lax.fori_loop(0, count, step, 0)
        for r in range(count):
            for ec in range(2):
                near(r, ec, over_half, up_recv).wait_send()
        for k in range(count - slots0, count):
            free0(k)
        landed(o_ref.at[line(1) * 2], recv_sem.at[RECV[("out0",)]])
        landed(o_ref.at[x * 2 + 1], recv_sem.at[RECV[("out1",)]])
        landed(o_ref.at[line(1) * 2 + 1], recv_sem.at[RECV[("out2",)]])
        for cp in log:
            cp.wait_send()


def routed(sizes, anomaly_x, anomaly_y):
    rows, planes, lines, layers = sizes
    _, height, depth_x = anomaly_x.shape
    width, depth_y = anomaly_y.shape[1:]
    members = depth_y * rows * layers
    chunk, slots0, slots1 = height // 8, 4, 3
    count = height // chunk
    dma = pltpu.SemaphoreType.DMA
    any_ = pl.BlockSpec(memory_space=pl.ANY)
    kind = anomaly_x.dtype
    return pl.pallas_call(
        functools.partial(kernel, sizes),
        out_shape=jax.ShapeDtypeStruct((planes, height, width), jnp.bfloat16),
        in_specs=[any_, any_],
        out_specs=any_,
        scratch_shapes=[
            pltpu.VMEM((2, height, members), kind),
            pltpu.VMEM((lines * width, members), kind),
            pltpu.VMEM((2 * lines * width, members), kind),
            pltpu.VMEM((slots0, chunk, lines * width), jnp.bfloat16),
            pltpu.VMEM((slots1, chunk, 2 * lines * width), jnp.bfloat16),
            dma((4,)), dma((SENDS,)), dma((len(RECV),)),
            dma((2 * count,)), dma((2 * count,)), dma((2 * count,)), dma((2 * count,)), dma((2 * count,)), dma((2 * count,)),
            dma((slots0,)), dma((slots0,)), dma((3 * slots1,)), dma((slots1,)),
        ],
        compiler_params=pltpu.CompilerParams(
            collective_id=0, has_side_effects=True, vmem_limit_bytes=67043328
        ),
    )(anomaly_x, anomaly_y)


def on_device(mesh, anomaly_x, anomaly_y):
    rows, cols, layers = (mesh.shape[name] for name in ("row", "col", "layer"))
    batches, height, depth_x = anomaly_x.shape
    planes = batches // layers
    fits = rows == 2 and layers == 2 and batches == 8 and cols == 2 * planes
    if not fits or depth_x % LANES or height % 128:
        return gathered(anomaly_x, anomaly_y)
    return routed((rows, planes, cols // planes, layers), anomaly_x, anomaly_y)


def solution(mesh):
    placed = (P(None, "row", ("layer", "col")), P(None, "col", ("layer", "row")))
    return jax.shard_map(
        functools.partial(on_device, mesh),
        mesh=mesh, in_specs=placed, out_specs=P("layer", "row", "col"), check_vma=False,
    )
```

```python
import functools

import jax
import jax.numpy as jnp
from jax import lax
from jax.experimental import pallas as pl
from jax.experimental.pallas import tpu as pltpu
from jax.sharding import PartitionSpec as P

LANES = 128
MESH = pl.DeviceIdType.MESH
NT = (((1,), (1,)), ((), ()))


def gathered(anomaly_x, anomaly_y):
    panel_x = lax.all_gather(anomaly_x, "col", axis=2, tiled=True)
    partial_tile = jnp.einsum(
        "bik,bjk->bij",
        panel_x,
        lax.all_gather(anomaly_y, "row", axis=2, tiled=True),
        preferred_element_type=jnp.float32,
    )
    summed = lax.psum_scatter(partial_tile, "layer", scatter_dimension=0, tiled=True)
    return summed.astype(jnp.bfloat16)


def plan():
    recv = {}

    def add(*key):
        recv[key] = len(recv)

    for rel in range(4):
        for ec in range(2):
            for ex in range(2):
                if rel or ec or ex:
                    add("x0", rel, ec, ex)
    for ec in range(2):
        for ex in range(2):
            if ec or ex:
                add("x1", ec, ex)
            for yr in range(2):
                if ec or ex or yr:
                    add("y0", ec, ex, yr)
                    add("y1", 0, ec, ex, yr)
                add("y1", 1, ec, ex, yr)
    for kind in ("out0", "out1", "out2"):
        add(kind)
    return recv


RECV = plan()
SENDS = 48


def kernel(
    sizes, x_ref, y_ref, o_ref, xg, yg0, yg1, og0, og1,
    local_sem, send_sem, recv_sem, up_send, up_recv, near_send, far_send, near_recv, far_recv,
    o0_send, o0_keep, o1_send, o1_keep, acc,
):
    rows, planes, lines, layers = sizes
    y, col, c = lax.axis_index("row"), lax.axis_index("col"), lax.axis_index("layer")
    z, x = col // lines, lax.rem(col, lines)
    depth_x, depth_y = x_ref.shape[2], y_ref.shape[2]
    height, width = x_ref.shape[1], y_ref.shape[1]
    group = depth_x * planes * lines
    pair = depth_x * lines
    chunk = og0.shape[1]
    count = height // chunk
    slots0, slots1 = og0.shape[0], og1.shape[0]
    last, wide = count - 1, lines * width
    tails = [(0, chunk // 2), (chunk // 2, chunk // 4), (3 * chunk // 4, chunk // 4)]

    half = z // 2
    mid, end = 1 + half, 3 * half
    inner = (z == 1) | (z == 2)
    partner = z + 1 - 2 * lax.rem(z, 2)
    across = planes - 1 - z
    level = [z, partner, planes - 1 - mid, planes - 1 - end]

    def core(e):
        return lax.rem(c + e, layers)

    def line(e):
        return lax.rem(x + e, lines)

    def row(e):
        return lax.rem(y + e, rows)

    def dev(yy, zz, xx, cc):
        return {"row": yy, "col": zz * lines + xx, "layer": cc}

    def batch(ec, ex, s):
        return core(ec) * planes + line(ex) * 2 + s

    def xcols(rel, ec, ex):
        return pl.ds(pl.multiple_of(core(ec) * group + (level[rel] * lines + line(ex)) * depth_x, depth_x), depth_x)

    def xpair(rel, ec):
        return pl.ds(pl.multiple_of(core(ec) * group + level[rel] * pair, pair), pair)

    def ycols(ec, er):
        return pl.ds(pl.multiple_of(core(ec) * group + row(er) * depth_y, depth_y), depth_y)

    def y0zone(ec, ex, er):
        return yg0.at[pl.ds(pl.multiple_of(line(ex) * width, width), width), ycols(ec, er)]

    def y1zone(rel, ec, ex, er):
        at = lax.rem(level[rel], 2) * lines * width + line(ex) * width
        return yg1.at[pl.ds(pl.multiple_of(at, width), width), ycols(ec, er)]

    def rowsof(r):
        return pl.ds(pl.multiple_of(r * chunk, chunk), chunk)

    def tile(q):
        return pl.ds(pl.multiple_of(q * width, width), width)

    peers = [dev(y, z, line(ex), core(ec)) for ec in range(2) for ex in range(2) if ec or ex]
    peers += [dev(row(1), z, x, c), dev(y, partner, x, c), dev(y, partner, line(1), c), dev(y, across, x, c)]
    barrier = pltpu.get_barrier_semaphore()
    for peer in peers:
        pl.semaphore_signal(barrier, inc=1, device_id=peer, device_id_type=MESH)
    pl.semaphore_wait(barrier, len(peers))

    over_y, over_half, over_mid = dev(row(1), z, x, c), dev(y, partner, x, c), dev(y, across, x, c)

    def remote(src, dst, s, r, to):
        return pltpu.make_async_remote_copy(
            src_ref=src, dst_ref=dst, send_sem=s, recv_sem=r, device_id=to, device_id_type=MESH
        )

    def landed(dst, sem):
        remote(dst, dst, sem, sem, over_y).wait_recv()

    sent = []

    def push(log, src, dst, key, to):
        cp = remote(src, dst, send_sem.at[len(log)], recv_sem.at[RECV[key]], to)
        cp.start()
        log.append(cp)

    def await_x0(rel, ec, ex):
        landed(xg.at[0, :, xcols(rel, ec, ex)], recv_sem.at[RECV["x0", rel, ec, ex]])

    def await_x1(ec, ex):
        landed(xg.at[1, :, xcols(0, ec, ex)], recv_sem.at[RECV["x1", ec, ex]])

    def await_y0(ec, ex, er):
        landed(y0zone(ec, ex, er), recv_sem.at[RECV["y0", ec, ex, er]])

    def await_y1(rel, ec, ex, er):
        landed(y1zone(rel, ec, ex, er), recv_sem.at[RECV["y1", rel, ec, ex, er]])

    def send_x0(log, rel, ec, ex, to, there):
        zone = xg.at[0, :, xcols(rel, ec, ex)]
        src = zone if rel or ec or ex else x_ref.at[batch(0, 0, 0)]
        push(log, src, zone, ("x0", there, ec, ex), to)

    def send_y0(log, ec, ex):
        zone = y0zone(ec, ex, 0)
        src = zone if ec or ex else y_ref.at[batch(0, 0, 0)]
        push(log, src, zone, ("y0", ec, ex, 1), over_y)

    def send_y1(log, rel, ec, ex, to, there, er):
        zone = y1zone(rel, ec, ex, 0)
        src = zone if rel or ec or ex else y_ref.at[batch(0, 0, 1)]
        push(log, src, zone, ("y1", there, ec, ex, er), to)

    def spread(ec, ex):
        to = dev(y, z, line(ex), core(ec))
        own = (0, 0)
        push(sent, x_ref.at[batch(ec, ex, 0)], xg.at[0, :, xcols(0, *own)], ("x0", 0, ec, ex), to)
        push(sent, y_ref.at[batch(ec, ex, 1)], y1zone(0, *own, 0), ("y1", 0, ec, ex, 0), to)
        push(sent, x_ref.at[batch(ec, ex, 1)], xg.at[1, :, xcols(0, *own)], ("x1", ec, ex), to)
        push(sent, y_ref.at[batch(ec, ex, 0)], y0zone(*own, 0), ("y0", ec, ex, 0), to)

    def spread_line():
        own = (0, 0)
        for what in range(4):
            for ec in range(2):
                to = dev(y, z, line(1), core(ec))
                if what == 0:
                    push(sent, x_ref.at[batch(ec, 1, 0)], xg.at[0, :, xcols(0, *own)], ("x0", 0, ec, 1), to)
                elif what == 1:
                    push(sent, y_ref.at[batch(ec, 1, 1)], y1zone(0, *own, 0), ("y1", 0, ec, 1, 0), to)
                elif what == 2:
                    push(sent, x_ref.at[batch(ec, 1, 1)], xg.at[1, :, xcols(0, *own)], ("x1", ec, 1), to)
                else:
                    push(sent, y_ref.at[batch(ec, 1, 0)], y0zone(*own, 0), ("y0", ec, 1, 0), to)

    send_x0(sent, 0, 0, 0, over_half, 1)
    spread(1, 0)
    spread_line()
    keeps = [
        pltpu.make_async_copy(x_ref.at[batch(0, 0, s)], xg.at[s, :, xcols(0, 0, 0)], local_sem.at[s]) for s in range(2)
    ] + [
        pltpu.make_async_copy(y_ref.at[batch(0, 0, 0)], y0zone(0, 0, 0), local_sem.at[2]),
        pltpu.make_async_copy(y_ref.at[batch(0, 0, 1)], y1zone(0, 0, 0, 0), local_sem.at[3]),
    ]
    for keep in keeps:
        keep.start()

    def out0(k, e):
        slot = lax.rem(k, slots0)
        src = og0.at[slot, :, tile(line(e))]
        dst = o_ref.at[x * 2, rowsof(k)]
        if e == 0:
            return pltpu.make_async_copy(src, dst, o0_keep.at[slot])
        return remote(src, dst, o0_send.at[slot], recv_sem.at[RECV[("out0",)]], dev(y, z, line(1), c))

    def free0(k):
        out0(k, 0).wait()
        out0(k, 1).wait_send()

    def product0(k):
        pl.when(k >= slots0)(lambda: free0(k - slots0))
        og0[lax.rem(k, slots0)] = lax.dot_general(
            xg[0, rowsof(k), :], yg0[...], NT, preferred_element_type=jnp.float32
        ).astype(jnp.bfloat16)
        out0(k, 0).start()
        out0(k, 1).start()

    def out1(r, ez, ex):
        slot = lax.rem(r, slots1)
        zz = lax.rem(level[ez], 2)
        src = og1.at[slot, :, tile(zz * lines + line(ex))]
        dst = o_ref.at[x * 2 + 1, rowsof(r)]
        if not ez and not ex:
            return pltpu.make_async_copy(src, dst, o1_keep.at[slot])
        kind = "out1" if ez == 0 or ex == 0 else "out2"
        return remote(src, dst, o1_send.at[slot * 3 + ez * 2 + ex - 1], recv_sem.at[RECV[(kind,)]],
                      dev(y, level[ez], line(ex), c))

    def free1(r):
        out1(r, 0, 0).wait()
        for ez, ex in ((1, 1), (1, 0), (0, 1)):
            out1(r, ez, ex).wait_send()

    def near(r, ec, to, sems):
        zone = xg.at[1, rowsof(r), xpair(0, ec)]
        return remote(zone, zone, near_send.at[r * 2 + ec], sems.at[r * 2 + ec], to)

    def far(r, ec):
        zone = xg.at[1, rowsof(r), xpair(1, ec)]
        return remote(zone, zone, far_send.at[r * 2 + ec], far_recv.at[r * 2 + ec], over_mid)

    def send_near(r):
        for ec in range(2):
            near(r, ec, over_mid, near_recv).start()

    def far_tail(j, ec):
        at, size = tails[j]
        zone = xg.at[1, pl.ds(last * chunk + at, size), xpair(1, ec)]
        k = (last + j) * 2 + ec
        return remote(zone, zone, far_send.at[k], far_recv.at[k], over_mid)

    def send_far(r):
        for ec in range(2):
            landed(xg.at[1, rowsof(r), xpair(1, ec)], up_recv.at[r * 2 + ec])
            far(r, ec).start()

    def send_tails():
        for ec in range(2):
            landed(xg.at[1, rowsof(last), xpair(1, ec)], up_recv.at[last * 2 + ec])
        for j in range(len(tails)):
            for ec in range(2):
                far_tail(j, ec).start()

    def product1(r):
        for ec in range(2):
            landed(xg.at[1, rowsof(r), xpair(2, ec)], near_recv.at[r * 2 + ec])
            landed(xg.at[1, rowsof(r), xpair(3, ec)], far_recv.at[r * 2 + ec])
        pl.when(r >= slots1)(lambda: free1(r - slots1))
        slot = lax.rem(r, slots1)

        def part(q, _):
            at = pl.ds(pl.multiple_of(q * wide, wide), wide)
            og1[slot, :, at] = lax.dot_general(
                xg[1, rowsof(r), :], yg1[at, :], NT, preferred_element_type=jnp.float32
            ).astype(jnp.bfloat16)
            return 0

        lax.fori_loop(0, 2, part, 0)
        for ez, ex in ((1, 1), (1, 0), (0, 1), (0, 0)):
            out1(r, ez, ex).start()

    def out_tail(j, ez, ex):
        at, size = tails[j]
        zz = lax.rem(level[ez], 2)
        src = og1.at[last % slots1, pl.ds(at, size), tile(zz * lines + line(ex))]
        dst = o_ref.at[x * 2 + 1, pl.ds(last * chunk + at, size)]
        if not ez and not ex:
            return pltpu.make_async_copy(src, dst, o1_keep.at[slots1 + j])
        kind = "out1" if ez == 0 or ex == 0 else "out2"
        return remote(src, dst, o1_send.at[(slots1 + j) * 3 + ez * 2 + ex - 1], recv_sem.at[RECV[(kind,)]],
                      dev(y, level[ez], line(ex), c))

    def members(ec, far_part):
        third = planes - 1
        if far_part:
            return xpair(3, ec)
        first = jnp.where(level[3] == 0, pair, 0)
        return pl.ds(pl.multiple_of(core(ec) * group + first, pair), third * pair)

    def terms(rows_at, cols_at, far_part):
        total = None
        for ec in range(2):
            at = members(ec, far_part)
            term = lax.dot_general(xg[1, rows_at, at], yg1[cols_at, at], NT, preferred_element_type=jnp.float32)
            total = term if total is None else total + term
        return total

    def half_cols(q):
        return pl.ds(pl.multiple_of(q * wide, wide), wide)

    def product_last():
        for ec in range(2):
            landed(xg.at[1, rowsof(last), xpair(2, ec)], near_recv.at[last * 2 + ec])

        def part(q, _):
            acc[:, half_cols(q)] = terms(rowsof(last), half_cols(q), False)
            return 0

        lax.fori_loop(0, 2, part, 0)
        free1(last - slots1)
        for j, (at, size) in enumerate(tails):
            for ec in range(2):
                landed(xg.at[1, pl.ds(last * chunk + at, size), xpair(3, ec)], far_recv.at[(last + j) * 2 + ec])
            for ez in (1, 0):
                cols_at = half_cols(lax.rem(level[ez], 2))
                og1[last % slots1, pl.ds(at, size), cols_at] = (
                    acc[pl.ds(at, size), cols_at] + terms(pl.ds(last * chunk + at, size), cols_at, True)
                ).astype(jnp.bfloat16)
                for ex in (1, 0):
                    out_tail(j, ez, ex).start()

    ahead = 4

    @pl.when(inner)
    def _():
        log = list(sent)
        send_x0(log, 0, 0, 0, over_mid, 2)
        send_y1(log, 0, 0, 0, over_y, 0, 1)

        def own(ec, ex):
            await_x0(0, ec, ex)
            send_x0(log, 0, ec, ex, over_mid, 2)
            send_x0(log, 0, ec, ex, over_half, 1)

        def outer(ec, ex):
            await_x0(1, ec, ex)
            send_x0(log, 1, ec, ex, over_mid, 3)

        def other(rel, ec, ex):
            await_x0(rel, ec, ex)
            send_x0(log, rel, ec, ex, over_half, rel)

        def side0(ec, ex):
            await_y0(ec, ex, 0)
            send_y0(log, ec, ex)

        def side1(rel, ec, ex):
            await_y1(rel, ec, ex, 0)
            send_y1(log, rel, ec, ex, over_y, rel, 1)

        own(1, 0)
        side1(0, 1, 0)
        send_y0(log, 0, 0)
        own(0, 1)
        outer(0, 0)
        other(2, 0, 0)
        own(1, 1)
        outer(1, 0)
        other(2, 1, 0)
        side1(0, 0, 1)
        other(2, 0, 1)
        side1(1, 0, 0)
        side1(0, 1, 1)
        side1(1, 1, 0)
        side0(1, 0)
        other(2, 1, 1)
        outer(0, 1)
        other(3, 0, 0)
        outer(1, 1)
        other(3, 1, 0)
        keeps[1].wait()
        await_x1(1, 0)
        await_x1(0, 1)
        await_x1(1, 1)
        send_near(0)
        send_near(1)
        side1(1, 0, 1)
        other(3, 0, 1)
        side0(0, 1)
        side1(1, 1, 1)
        other(3, 1, 1)
        side0(1, 1)
        for r in range(ahead):
            send_far(r)
            send_near(r + 2)
        keeps[0].wait()
        keeps[2].wait()
        keeps[3].wait()
        for rel in range(2):
            for ec in range(2):
                for ex in range(2):
                    await_y1(rel, ec, ex, 1)

        def both(r, _):
            product1(r)

            @pl.when(r + ahead < last)
            def _():
                send_far(r + ahead)

            @pl.when(r == 0)
            def _():
                send_near(last - 1)

            @pl.when(r == 2)
            def _():
                send_near(last)

            @pl.when(r + ahead == last)
            def _():
                send_tails()

            @pl.when(r == 3)
            def _():
                for ec in range(2):
                    for ex in range(2):
                        await_y0(ec, ex, 1)

            @pl.when((r >= 3) & (r < 7))
            def _():
                def step(k, _):
                    product0((r - 3) * (count // 4) + k)
                    return 0

                lax.fori_loop(0, count // 4, step, 0)

            return 0

        lax.fori_loop(0, last, both, 0)
        product_last()
        for r in range(count):
            for ec in range(2):
                near(r, ec, over_mid, near_recv).wait_send()
                if r < last:
                    far(r, ec).wait_send()
        for j in range(len(tails)):
            for ec in range(2):
                far_tail(j, ec).wait_send()
            for ez, ex in ((1, 1), (1, 0), (0, 1)):
                out_tail(j, ez, ex).wait_send()
            out_tail(j, 0, 0).wait()
        for r in range(count - slots1, last):
            free1(r)
        for k in range(count - slots0, count):
            free0(k)
        landed(o_ref.at[line(1) * 2], recv_sem.at[RECV[("out0",)]])
        landed(o_ref.at[line(1) * 2 + 1], recv_sem.at[RECV[("out1",)]])
        for cp in log:
            cp.wait_send()

    @pl.when(jnp.logical_not(inner))
    def _():
        log = list(sent)

        def own(ec, ex):
            await_x0(0, ec, ex)
            send_x0(log, 0, ec, ex, over_half, 1)

        def side0(ec, ex):
            await_y0(ec, ex, 0)
            send_y0(log, ec, ex)

        def down(ec, ex):
            if ec or ex:
                await_y1(0, ec, ex, 0)
            send_y1(log, 0, ec, ex, over_half, 1, 0)

        own(1, 0)
        down(0, 0)
        down(1, 0)
        send_y0(log, 0, 0)
        side0(1, 0)
        own(0, 1)
        own(1, 1)
        down(0, 1)
        down(1, 1)
        keeps[1].wait()
        await_x1(1, 0)
        await_x1(0, 1)
        await_x1(1, 1)
        for r in range(count):
            for ec in range(2):
                near(r, ec, over_half, up_recv).start()
        side0(0, 1)
        side0(1, 1)
        keeps[0].wait()
        keeps[2].wait()
        keeps[3].wait()
        for ec in range(2):
            for ex in range(2):
                await_y0(ec, ex, 1)
        for rel in range(1, 4):
            for ec in range(2):
                for ex in range(2):
                    await_x0(rel, ec, ex)

        def step(k, _):
            product0(k)
            return 0

        lax.fori_loop(0, count, step, 0)
        for r in range(count):
            for ec in range(2):
                near(r, ec, over_half, up_recv).wait_send()
        for k in range(count - slots0, count):
            free0(k)
        landed(o_ref.at[line(1) * 2], recv_sem.at[RECV[("out0",)]])
        landed(o_ref.at[x * 2 + 1], recv_sem.at[RECV[("out1",)]])
        landed(o_ref.at[line(1) * 2 + 1], recv_sem.at[RECV[("out2",)]])
        for cp in log:
            cp.wait_send()


def routed(sizes, anomaly_x, anomaly_y):
    rows, planes, lines, layers = sizes
    _, height, depth_x = anomaly_x.shape
    width, depth_y = anomaly_y.shape[1:]
    members = depth_y * rows * layers
    chunk, slots0, slots1 = height // 8, 2, 2
    count = height // chunk
    dma = pltpu.SemaphoreType.DMA
    any_ = pl.BlockSpec(memory_space=pl.ANY)
    kind = anomaly_x.dtype
    return pl.pallas_call(
        functools.partial(kernel, sizes),
        out_shape=jax.ShapeDtypeStruct((planes, height, width), jnp.bfloat16),
        in_specs=[any_, any_],
        out_specs=any_,
        scratch_shapes=[
            pltpu.VMEM((2, height, members), kind),
            pltpu.VMEM((lines * width, members), kind),
            pltpu.VMEM((2 * lines * width, members), kind),
            pltpu.VMEM((slots0, chunk, lines * width), jnp.bfloat16),
            pltpu.VMEM((slots1, chunk, 2 * lines * width), jnp.bfloat16),
            dma((4,)), dma((SENDS,)), dma((len(RECV),)),
            dma((2 * count,)), dma((2 * count,)), dma((2 * count,)), dma((2 * count + 4,)), dma((2 * count,)), dma((2 * count + 4,)),
            dma((slots0,)), dma((slots0,)), dma((3 * slots1 + 9,)), dma((slots1 + 3,)),
            pltpu.VMEM((chunk, 2 * lines * width), jnp.float32),
        ],
        compiler_params=pltpu.CompilerParams(
            collective_id=0, has_side_effects=True, vmem_limit_bytes=67043328
        ),
    )(anomaly_x, anomaly_y)


def on_device(mesh, anomaly_x, anomaly_y):
    rows, cols, layers = (mesh.shape[name] for name in ("row", "col", "layer"))
    batches, height, depth_x = anomaly_x.shape
    planes = batches // layers
    fits = rows == 2 and layers == 2 and batches == 8 and cols == 2 * planes
    if not fits or depth_x % LANES or height % 128:
        return gathered(anomaly_x, anomaly_y)
    return routed((rows, planes, cols // planes, layers), anomaly_x, anomaly_y)


def solution(mesh):
    placed = (P(None, "row", ("layer", "col")), P(None, "col", ("layer", "row")))
    return jax.shard_map(
        functools.partial(on_device, mesh),
        mesh=mesh, in_specs=placed, out_specs=P("layer", "row", "col"), check_vma=False,
    )
```

```python
import functools

import jax
import jax.numpy as jnp
from jax import lax
from jax.experimental import pallas as pl
from jax.experimental.pallas import tpu as pltpu
from jax.sharding import PartitionSpec as P

LANES = 128
MESH = pl.DeviceIdType.MESH
NT = (((1,), (1,)), ((), ()))


def gathered(anomaly_x, anomaly_y):
    panel_x = lax.all_gather(anomaly_x, "col", axis=2, tiled=True)
    partial_tile = jnp.einsum(
        "bik,bjk->bij",
        panel_x,
        lax.all_gather(anomaly_y, "row", axis=2, tiled=True),
        preferred_element_type=jnp.float32,
    )
    summed = lax.psum_scatter(partial_tile, "layer", scatter_dimension=0, tiled=True)
    return summed.astype(jnp.bfloat16)


HALVES = 2


def plan():
    recv = {}

    def add(*key):
        recv[key] = len(recv)

    for rel in range(4):
        for ec in range(2):
            for ex in range(2):
                for h in range(HALVES):
                    if rel or ec or ex:
                        add("x0", rel, ec, ex, h)
    for ec in range(2):
        for ex in range(2):
            if ec or ex:
                add("x1", ec, ex)
            for yr in range(2):
                if ec or ex or yr:
                    add("y0", ec, ex, yr)
                    add("y1", 0, ec, ex, yr)
                add("y1", 1, ec, ex, yr)
    for kind in ("out0", "out1", "out2"):
        add(kind)
    return recv


RECV = plan()
SENDS = 80


def kernel(
    sizes, x_ref, y_ref, o_ref, xg, yg0, yg1, og0, og1,
    local_sem, send_sem, recv_sem, up_send, up_recv, near_send, far_send, near_recv, far_recv,
    o0_send, o0_keep, o1_send, o1_keep, acc,
):
    rows, planes, lines, layers = sizes
    y, col, c = lax.axis_index("row"), lax.axis_index("col"), lax.axis_index("layer")
    z, x = col // lines, lax.rem(col, lines)
    depth_x, depth_y = x_ref.shape[2], y_ref.shape[2]
    height, width = x_ref.shape[1], y_ref.shape[1]
    group = depth_x * planes * lines
    pair = depth_x * lines
    chunk = og0.shape[1]
    count = height // chunk
    slots0, slots1 = og0.shape[0], og1.shape[0]
    last, wide = count - 1, lines * width
    tails = [(j * chunk // 4, chunk // 4) for j in range(4)]

    half = z // 2
    mid, end = 1 + half, 3 * half
    inner = (z == 1) | (z == 2)
    partner = z + 1 - 2 * lax.rem(z, 2)
    across = planes - 1 - z
    level = [z, partner, planes - 1 - mid, planes - 1 - end]

    def core(e):
        return lax.rem(c + e, layers)

    def line(e):
        return lax.rem(x + e, lines)

    def row(e):
        return lax.rem(y + e, rows)

    def dev(yy, zz, xx, cc):
        return {"row": yy, "col": zz * lines + xx, "layer": cc}

    def batch(ec, ex, s):
        return core(ec) * planes + line(ex) * 2 + s

    def xcols(rel, ec, ex):
        return pl.ds(pl.multiple_of(core(ec) * group + (level[rel] * lines + line(ex)) * depth_x, depth_x), depth_x)

    def xpair(rel, ec):
        return pl.ds(pl.multiple_of(core(ec) * group + level[rel] * pair, pair), pair)

    def ycols(ec, er):
        return pl.ds(pl.multiple_of(core(ec) * group + row(er) * depth_y, depth_y), depth_y)

    def y0zone(ec, ex, er):
        return yg0.at[pl.ds(pl.multiple_of(line(ex) * width, width), width), ycols(ec, er)]

    def y1zone(rel, ec, ex, er):
        at = lax.rem(level[rel], 2) * lines * width + line(ex) * width
        return yg1.at[pl.ds(pl.multiple_of(at, width), width), ycols(ec, er)]

    def half_rows(h):
        return pl.ds(h * (height // HALVES), height // HALVES)

    def rowsof(r):
        return pl.ds(pl.multiple_of(r * chunk, chunk), chunk)

    def tile(q):
        return pl.ds(pl.multiple_of(q * width, width), width)

    peers = [dev(y, z, line(ex), core(ec)) for ec in range(2) for ex in range(2) if ec or ex]
    peers += [dev(row(1), z, x, c), dev(y, partner, x, c), dev(y, partner, line(1), c), dev(y, across, x, c)]
    barrier = pltpu.get_barrier_semaphore()
    for peer in peers:
        pl.semaphore_signal(barrier, inc=1, device_id=peer, device_id_type=MESH)
    pl.semaphore_wait(barrier, len(peers))

    over_y, over_half, over_mid = dev(row(1), z, x, c), dev(y, partner, x, c), dev(y, across, x, c)

    def remote(src, dst, s, r, to):
        return pltpu.make_async_remote_copy(
            src_ref=src, dst_ref=dst, send_sem=s, recv_sem=r, device_id=to, device_id_type=MESH
        )

    def landed(dst, sem):
        remote(dst, dst, sem, sem, over_y).wait_recv()

    sent = []

    def push(log, src, dst, key, to):
        cp = remote(src, dst, send_sem.at[len(log)], recv_sem.at[RECV[key]], to)
        cp.start()
        log.append(cp)

    def await_x0(rel, ec, ex, h):
        landed(xg.at[0, half_rows(h), xcols(rel, ec, ex)], recv_sem.at[RECV["x0", rel, ec, ex, h]])

    def await_x1(ec, ex):
        landed(xg.at[1, :, xcols(0, ec, ex)], recv_sem.at[RECV["x1", ec, ex]])

    def await_y0(ec, ex, er):
        landed(y0zone(ec, ex, er), recv_sem.at[RECV["y0", ec, ex, er]])

    def await_y1(rel, ec, ex, er):
        landed(y1zone(rel, ec, ex, er), recv_sem.at[RECV["y1", rel, ec, ex, er]])

    def send_x0(log, rel, ec, ex, h, to, there):
        zone = xg.at[0, half_rows(h), xcols(rel, ec, ex)]
        src = zone if rel or ec or ex else x_ref.at[batch(0, 0, 0), half_rows(h)]
        push(log, src, zone, ("x0", there, ec, ex, h), to)

    def send_y0(log, ec, ex):
        zone = y0zone(ec, ex, 0)
        src = zone if ec or ex else y_ref.at[batch(0, 0, 0)]
        push(log, src, zone, ("y0", ec, ex, 1), over_y)

    def send_y1(log, rel, ec, ex, to, there, er):
        zone = y1zone(rel, ec, ex, 0)
        src = zone if rel or ec or ex else y_ref.at[batch(0, 0, 1)]
        push(log, src, zone, ("y1", there, ec, ex, er), to)

    def spread(ec, ex, what, h=0):
        to = dev(y, z, line(ex), core(ec))
        if what == "x0":
            push(sent, x_ref.at[batch(ec, ex, 0), half_rows(h)], xg.at[0, half_rows(h), xcols(0, 0, 0)],
                 ("x0", 0, ec, ex, h), to)
        elif what == "y1":
            push(sent, y_ref.at[batch(ec, ex, 1)], y1zone(0, 0, 0, 0), ("y1", 0, ec, ex, 0), to)
        elif what == "x1":
            push(sent, x_ref.at[batch(ec, ex, 1)], xg.at[1, :, xcols(0, 0, 0)], ("x1", ec, ex), to)
        else:
            push(sent, y_ref.at[batch(ec, ex, 0)], y0zone(0, 0, 0), ("y0", ec, ex, 0), to)

    send_x0(sent, 0, 0, 0, 0, over_half, 1)
    for targets in (((1, 0),), ((0, 1), (1, 1))):
        for h in range(HALVES):
            for ec, ex in targets:
                spread(ec, ex, "x0", h)
        for what in ("y1", "x1", "y0"):
            for ec, ex in targets:
                spread(ec, ex, what)
    keeps = [
        pltpu.make_async_copy(x_ref.at[batch(0, 0, s)], xg.at[s, :, xcols(0, 0, 0)], local_sem.at[s]) for s in range(2)
    ] + [
        pltpu.make_async_copy(y_ref.at[batch(0, 0, 0)], y0zone(0, 0, 0), local_sem.at[2]),
        pltpu.make_async_copy(y_ref.at[batch(0, 0, 1)], y1zone(0, 0, 0, 0), local_sem.at[3]),
    ]
    for keep in keeps:
        keep.start()

    def out0(k, e):
        slot = lax.rem(k, slots0)
        src = og0.at[slot, :, tile(line(e))]
        dst = o_ref.at[x * 2, rowsof(k)]
        if e == 0:
            return pltpu.make_async_copy(src, dst, o0_keep.at[slot])
        return remote(src, dst, o0_send.at[slot], recv_sem.at[RECV[("out0",)]], dev(y, z, line(1), c))

    def free0(k):
        out0(k, 0).wait()
        out0(k, 1).wait_send()

    def product0(k):
        pl.when(k >= slots0)(lambda: free0(k - slots0))
        og0[lax.rem(k, slots0)] = lax.dot_general(
            xg[0, rowsof(k), :], yg0[...], NT, preferred_element_type=jnp.float32
        ).astype(jnp.bfloat16)
        out0(k, 0).start()
        out0(k, 1).start()

    def out1(r, ez, ex):
        slot = lax.rem(r, slots1)
        zz = lax.rem(level[ez], 2)
        src = og1.at[slot, :, tile(zz * lines + line(ex))]
        dst = o_ref.at[x * 2 + 1, rowsof(r)]
        if not ez and not ex:
            return pltpu.make_async_copy(src, dst, o1_keep.at[slot])
        kind = "out1" if ez == 0 or ex == 0 else "out2"
        return remote(src, dst, o1_send.at[slot * 3 + ez * 2 + ex - 1], recv_sem.at[RECV[(kind,)]],
                      dev(y, level[ez], line(ex), c))

    def free1(r):
        out1(r, 0, 0).wait()
        for ez, ex in ((1, 1), (1, 0), (0, 1)):
            out1(r, ez, ex).wait_send()

    def near(r, ec, to, sems):
        zone = xg.at[1, rowsof(r), xpair(0, ec)]
        return remote(zone, zone, near_send.at[r * 2 + ec], sems.at[r * 2 + ec], to)

    def far(r, ec):
        zone = xg.at[1, rowsof(r), xpair(1, ec)]
        return remote(zone, zone, far_send.at[r * 2 + ec], far_recv.at[r * 2 + ec], over_mid)

    def send_near(r):
        for ec in range(2):
            near(r, ec, over_mid, near_recv).start()

    def far_tail(j, ec):
        at, size = tails[j]
        zone = xg.at[1, pl.ds(last * chunk + at, size), xpair(1, ec)]
        k = (last + j) * 2 + ec
        return remote(zone, zone, far_send.at[k], far_recv.at[k], over_mid)

    def send_far(r):
        for ec in range(2):
            landed(xg.at[1, rowsof(r), xpair(1, ec)], up_recv.at[r * 2 + ec])
            far(r, ec).start()

    def send_tails():
        for ec in range(2):
            landed(xg.at[1, rowsof(last), xpair(1, ec)], up_recv.at[last * 2 + ec])
        for j in range(len(tails)):
            for ec in range(2):
                far_tail(j, ec).start()

    def product1(r):
        for ec in range(2):
            landed(xg.at[1, rowsof(r), xpair(2, ec)], near_recv.at[r * 2 + ec])
            landed(xg.at[1, rowsof(r), xpair(3, ec)], far_recv.at[r * 2 + ec])
        pl.when(r >= slots1)(lambda: free1(r - slots1))
        slot = lax.rem(r, slots1)

        def part(q, _):
            at = pl.ds(pl.multiple_of(q * wide, wide), wide)
            og1[slot, :, at] = lax.dot_general(
                xg[1, rowsof(r), :], yg1[at, :], NT, preferred_element_type=jnp.float32
            ).astype(jnp.bfloat16)
            return 0

        lax.fori_loop(0, 2, part, 0)
        for ez, ex in ((1, 1), (1, 0), (0, 1), (0, 0)):
            out1(r, ez, ex).start()

    def out_tail(j, ez, ex):
        at, size = tails[j]
        zz = lax.rem(level[ez], 2)
        src = og1.at[last % slots1, pl.ds(at, size), tile(zz * lines + line(ex))]
        dst = o_ref.at[x * 2 + 1, pl.ds(last * chunk + at, size)]
        if not ez and not ex:
            return pltpu.make_async_copy(src, dst, o1_keep.at[slots1 + j])
        kind = "out1" if ez == 0 or ex == 0 else "out2"
        return remote(src, dst, o1_send.at[(slots1 + j) * 3 + ez * 2 + ex - 1], recv_sem.at[RECV[(kind,)]],
                      dev(y, level[ez], line(ex), c))

    def members(ec, far_part):
        third = planes - 1
        if far_part:
            return xpair(3, ec)
        first = jnp.where(level[3] == 0, pair, 0)
        return pl.ds(pl.multiple_of(core(ec) * group + first, pair), third * pair)

    def terms(rows_at, cols_at, far_part):
        total = None
        for ec in range(2):
            at = members(ec, far_part)
            term = lax.dot_general(xg[1, rows_at, at], yg1[cols_at, at], NT, preferred_element_type=jnp.float32)
            total = term if total is None else total + term
        return total

    def half_cols(q):
        return pl.ds(pl.multiple_of(q * wide, wide), wide)

    def product_last():
        for ec in range(2):
            landed(xg.at[1, rowsof(last), xpair(2, ec)], near_recv.at[last * 2 + ec])

        def part(q, _):
            acc[:, half_cols(q)] = terms(rowsof(last), half_cols(q), False)
            return 0

        lax.fori_loop(0, 2, part, 0)
        free1(last - slots1)
        for j, (at, size) in enumerate(tails):
            for ec in range(2):
                landed(xg.at[1, pl.ds(last * chunk + at, size), xpair(3, ec)], far_recv.at[(last + j) * 2 + ec])
            for ez in (1, 0):
                cols_at = half_cols(lax.rem(level[ez], 2))
                og1[last % slots1, pl.ds(at, size), cols_at] = (
                    acc[pl.ds(at, size), cols_at] + terms(pl.ds(last * chunk + at, size), cols_at, True)
                ).astype(jnp.bfloat16)
                for ex in (1, 0):
                    out_tail(j, ez, ex).start()

    ahead = 4

    @pl.when(inner)
    def _():
        log = list(sent)
        send_x0(log, 0, 0, 0, 0, over_mid, 2)
        send_y1(log, 0, 0, 0, over_y, 0, 1)

        def own_mid(ec, ex, h):
            if ec or ex:
                await_x0(0, ec, ex, h)
            send_x0(log, 0, ec, ex, h, over_mid, 2)

        def own_half(ec, ex, h):
            send_x0(log, 0, ec, ex, h, over_half, 1)

        def outer(ec, ex, h):
            await_x0(1, ec, ex, h)
            send_x0(log, 1, ec, ex, h, over_mid, 3)

        def other(rel, ec, ex, h):
            await_x0(rel, ec, ex, h)
            send_x0(log, rel, ec, ex, h, over_half, rel)

        def side0(ec, ex):
            await_y0(ec, ex, 0)
            send_y0(log, ec, ex)

        def side1(rel, ec, ex):
            await_y1(rel, ec, ex, 0)
            send_y1(log, rel, ec, ex, over_y, rel, 1)

        own_mid(1, 0, 0)
        own_half(1, 0, 0)
        side1(0, 1, 0)
        send_y0(log, 0, 0)
        side0(1, 0)
        for ex_ec in ((0, 1), (1, 1)):
            own_mid(*ex_ec, 0)
            own_half(*ex_ec, 0)
        every = ((0, 0), (1, 0), (0, 1), (1, 1))
        for at in every:
            outer(*at, 0)
            other(2, *at, 0)
        for at in every:
            own_mid(*at, 1)
        other(3, 0, 0, 0)
        outer(0, 0, 1)
        other(3, 1, 0, 0)
        outer(1, 0, 1)
        side1(0, 0, 1)
        other(3, 0, 1, 0)
        outer(0, 1, 1)
        other(3, 1, 1, 0)
        outer(1, 1, 1)
        for at in every:
            own_half(*at, 1)
        side1(0, 1, 1)
        other(2, 0, 0, 1)
        side1(1, 0, 0)
        other(2, 1, 0, 1)
        other(2, 0, 1, 1)
        other(2, 1, 1, 1)
        side1(1, 1, 0)
        keeps[1].wait()
        await_x1(1, 0)
        await_x1(0, 1)
        await_x1(1, 1)
        send_near(0)
        send_near(1)
        other(3, 0, 0, 1)
        other(3, 1, 0, 1)
        side1(1, 0, 1)
        other(3, 0, 1, 1)
        side0(0, 1)
        other(3, 1, 1, 1)
        side1(1, 1, 1)
        side0(1, 1)
        for r in range(ahead):
            send_far(r)
            send_near(r + 2)
        keeps[0].wait()
        keeps[2].wait()
        keeps[3].wait()
        for rel in range(2):
            for ec in range(2):
                for ex in range(2):
                    await_y1(rel, ec, ex, 1)

        def both(r, _):
            product1(r)

            @pl.when(r + ahead < last)
            def _():
                send_far(r + ahead)

            @pl.when(r == 0)
            def _():
                send_near(last - 1)

            @pl.when(r == 2)
            def _():
                send_near(last)

            @pl.when(r + ahead == last)
            def _():
                send_tails()

            @pl.when(r == 2)
            def _():
                for ec in range(2):
                    for ex in range(2):
                        await_y0(ec, ex, 1)

            @pl.when((r >= 2) & (r < 6))
            def _():
                def step(k, _):
                    product0((r - 2) * (count // 4) + k)
                    return 0

                lax.fori_loop(0, count // 4, step, 0)

            return 0

        lax.fori_loop(0, last, both, 0)
        product_last()
        for r in range(count):
            for ec in range(2):
                near(r, ec, over_mid, near_recv).wait_send()
                if r < last:
                    far(r, ec).wait_send()
        for j in range(len(tails)):
            for ec in range(2):
                far_tail(j, ec).wait_send()
            for ez, ex in ((1, 1), (1, 0), (0, 1)):
                out_tail(j, ez, ex).wait_send()
            out_tail(j, 0, 0).wait()
        for r in range(count - slots1, last):
            free1(r)
        for k in range(count - slots0, count):
            free0(k)
        landed(o_ref.at[line(1) * 2], recv_sem.at[RECV[("out0",)]])
        landed(o_ref.at[line(1) * 2 + 1], recv_sem.at[RECV[("out1",)]])
        for cp in log:
            cp.wait_send()

    @pl.when(jnp.logical_not(inner))
    def _():
        log = list(sent)

        def own(ec, ex, h):
            if ec or ex:
                await_x0(0, ec, ex, h)
            send_x0(log, 0, ec, ex, h, over_half, 1)

        def side0(ec, ex):
            await_y0(ec, ex, 0)
            send_y0(log, ec, ex)

        def down(ec, ex):
            if ec or ex:
                await_y1(0, ec, ex, 0)
            send_y1(log, 0, ec, ex, over_half, 1, 0)

        own(1, 0, 0)
        send_y0(log, 0, 0)
        side0(1, 0)
        own(0, 1, 0)
        own(1, 1, 0)
        for at in ((0, 0), (1, 0), (0, 1), (1, 1)):
            own(*at, 1)
        for at in ((0, 0), (1, 0), (0, 1), (1, 1)):
            down(*at)
        keeps[1].wait()
        await_x1(1, 0)
        await_x1(0, 1)
        await_x1(1, 1)
        for r in range(count):
            for ec in range(2):
                near(r, ec, over_half, up_recv).start()
        side0(0, 1)
        side0(1, 1)
        keeps[0].wait()
        keeps[2].wait()
        keeps[3].wait()
        for ec in range(2):
            for ex in range(2):
                await_y0(ec, ex, 1)
        def step(k, _):
            @pl.when(lax.rem(k, count // HALVES) == 0)
            def _():
                for h in range(HALVES):
                    @pl.when(k == h * (count // HALVES))
                    def _():
                        for rel in range(1, 4):
                            for ec in range(2):
                                for ex in range(2):
                                    await_x0(rel, ec, ex, h)

            product0(k)
            return 0

        lax.fori_loop(0, count, step, 0)
        for r in range(count):
            for ec in range(2):
                near(r, ec, over_half, up_recv).wait_send()
        for k in range(count - slots0, count):
            free0(k)
        landed(o_ref.at[line(1) * 2], recv_sem.at[RECV[("out0",)]])
        landed(o_ref.at[x * 2 + 1], recv_sem.at[RECV[("out1",)]])
        landed(o_ref.at[line(1) * 2 + 1], recv_sem.at[RECV[("out2",)]])
        for cp in log:
            cp.wait_send()


def routed(sizes, anomaly_x, anomaly_y):
    rows, planes, lines, layers = sizes
    _, height, depth_x = anomaly_x.shape
    width, depth_y = anomaly_y.shape[1:]
    members = depth_y * rows * layers
    chunk, slots0, slots1 = height // 8, 2, 2
    count = height // chunk
    dma = pltpu.SemaphoreType.DMA
    any_ = pl.BlockSpec(memory_space=pl.ANY)
    kind = anomaly_x.dtype
    return pl.pallas_call(
        functools.partial(kernel, sizes),
        out_shape=jax.ShapeDtypeStruct((planes, height, width), jnp.bfloat16),
        in_specs=[any_, any_],
        out_specs=any_,
        scratch_shapes=[
            pltpu.VMEM((2, height, members), kind),
            pltpu.VMEM((lines * width, members), kind),
            pltpu.VMEM((2 * lines * width, members), kind),
            pltpu.VMEM((slots0, chunk, lines * width), jnp.bfloat16),
            pltpu.VMEM((slots1, chunk, 2 * lines * width), jnp.bfloat16),
            dma((4,)), dma((SENDS,)), dma((len(RECV),)),
            dma((2 * count,)), dma((2 * count,)), dma((2 * count,)), dma((2 * count + 6,)), dma((2 * count,)), dma((2 * count + 6,)),
            dma((slots0,)), dma((slots0,)), dma((3 * slots1 + 12,)), dma((slots1 + 4,)),
            pltpu.VMEM((chunk, 2 * lines * width), jnp.float32),
        ],
        compiler_params=pltpu.CompilerParams(
            collective_id=0, has_side_effects=True, vmem_limit_bytes=67043328
        ),
    )(anomaly_x, anomaly_y)


def on_device(mesh, anomaly_x, anomaly_y):
    rows, cols, layers = (mesh.shape[name] for name in ("row", "col", "layer"))
    batches, height, depth_x = anomaly_x.shape
    planes = batches // layers
    fits = rows == 2 and layers == 2 and batches == 8 and cols == 2 * planes
    if not fits or depth_x % LANES or height % 128:
        return gathered(anomaly_x, anomaly_y)
    return routed((rows, planes, cols // planes, layers), anomaly_x, anomaly_y)


def solution(mesh):
    placed = (P(None, "row", ("layer", "col")), P(None, "col", ("layer", "row")))
    return jax.shard_map(
        functools.partial(on_device, mesh),
        mesh=mesh, in_specs=placed, out_specs=P("layer", "row", "col"), check_vma=False,
    )
```

```python
import functools

import jax
import jax.numpy as jnp
from jax import lax
from jax.experimental import pallas as pl
from jax.experimental.pallas import tpu as pltpu
from jax.sharding import PartitionSpec as P

LANES = 128
MESH = pl.DeviceIdType.MESH
NT = (((1,), (1,)), ((), ()))


def gathered(anomaly_x, anomaly_y):
    panel_x = lax.all_gather(anomaly_x, "col", axis=2, tiled=True)
    partial_tile = jnp.einsum(
        "bik,bjk->bij",
        panel_x,
        lax.all_gather(anomaly_y, "row", axis=2, tiled=True),
        preferred_element_type=jnp.float32,
    )
    summed = lax.psum_scatter(partial_tile, "layer", scatter_dimension=0, tiled=True)
    return summed.astype(jnp.bfloat16)


HALVES = 2


def plan():
    recv = {}

    def add(*key):
        recv[key] = len(recv)

    for rel in range(4):
        for ec in range(2):
            for ex in range(2):
                for h in range(HALVES):
                    if rel or ec or ex:
                        add("x0", rel, ec, ex, h)
    for ec in range(2):
        for ex in range(2):
            if ec or ex:
                add("x1", ec, ex)
            for yr in range(2):
                if ec or ex or yr:
                    add("y0", ec, ex, yr)
                    add("y1", 0, ec, ex, yr)
                add("y1", 1, ec, ex, yr)
    for kind in ("out0", "out1", "out2"):
        add(kind)
    return recv


RECV = plan()
SENDS = 80


def kernel(
    sizes, x_ref, y_ref, o_ref, x0g, xg, xc, yg0, yg1, og0, og1, acc,
    local_sem, send_sem, recv_sem, up_send, up_recv, near_send, far_send, near_recv, far_recv, o0_send, o1_send,
):
    rows, planes, lines, layers = sizes
    y, col, c = lax.axis_index("row"), lax.axis_index("col"), lax.axis_index("layer")
    z, x = col // lines, lax.rem(col, lines)
    depth_x, depth_y = x_ref.shape[2], y_ref.shape[2]
    height, width = x_ref.shape[1], y_ref.shape[1]
    group = depth_x * planes * lines
    pair = depth_x * lines
    chunk = og0.shape[1]
    count = height // chunk
    slots0, slots1 = og0.shape[0], og1.shape[0]
    last, wide = count - 1, lines * width
    tails = [(j * chunk // 4, chunk // 4) for j in range(4)]

    half = z // 2
    mid, end = 1 + half, 3 * half
    inner = (z == 1) | (z == 2)
    partner = z + 1 - 2 * lax.rem(z, 2)
    across = planes - 1 - z
    level = [z, partner, planes - 1 - mid, planes - 1 - end]

    def core(e):
        return lax.rem(c + e, layers)

    def line(e):
        return lax.rem(x + e, lines)

    def row(e):
        return lax.rem(y + e, rows)

    def dev(yy, zz, xx, cc):
        return {"row": yy, "col": zz * lines + xx, "layer": cc}

    def batch(ec, ex, s):
        return core(ec) * planes + line(ex) * 2 + s

    def xcols(rel, ec, ex):
        return pl.ds(pl.multiple_of(core(ec) * group + (level[rel] * lines + line(ex)) * depth_x, depth_x), depth_x)

    def xpair(rel, ec):
        return pl.ds(pl.multiple_of(core(ec) * group + level[rel] * pair, pair), pair)

    def ycols(ec, er):
        return pl.ds(pl.multiple_of(core(ec) * group + row(er) * depth_y, depth_y), depth_y)

    def y0zone(ec, ex, er):
        return yg0.at[pl.ds(pl.multiple_of(line(ex) * width, width), width), ycols(ec, er)]

    def y1zone(rel, ec, ex, er):
        at = lax.rem(level[rel], 2) * lines * width + line(ex) * width
        return yg1.at[pl.ds(pl.multiple_of(at, width), width), ycols(ec, er)]

    def half_rows(h):
        return pl.ds(h * (height // HALVES), height // HALVES)

    def rowsof(r):
        return pl.ds(pl.multiple_of(r * chunk, chunk), chunk)

    def tile(q):
        return pl.ds(pl.multiple_of(q * width, width), width)

    peers = [dev(y, z, line(ex), core(ec)) for ec in range(2) for ex in range(2) if ec or ex]
    peers += [dev(row(1), z, x, c), dev(y, partner, x, c), dev(y, partner, line(1), c), dev(y, across, x, c)]
    barrier = pltpu.get_barrier_semaphore()
    for peer in peers:
        pl.semaphore_signal(barrier, inc=1, device_id=peer, device_id_type=MESH)
    pl.semaphore_wait(barrier, len(peers))

    over_y, over_half, over_mid = dev(row(1), z, x, c), dev(y, partner, x, c), dev(y, across, x, c)

    def remote(src, dst, s, r, to):
        return pltpu.make_async_remote_copy(
            src_ref=src, dst_ref=dst, send_sem=s, recv_sem=r, device_id=to, device_id_type=MESH
        )

    def landed(dst, sem):
        remote(dst, dst, sem, sem, over_y).wait_recv()

    sent = []

    def push(log, src, dst, key, to):
        cp = remote(src, dst, send_sem.at[len(log)], recv_sem.at[RECV[key]], to)
        cp.start()
        log.append(cp)

    def await_x0(rel, ec, ex, h):
        landed(x0g.at[half_rows(h), xcols(rel, ec, ex)], recv_sem.at[RECV["x0", rel, ec, ex, h]])

    def await_x1(ec, ex):
        landed(xg.at[:, xcols(0, ec, ex)], recv_sem.at[RECV["x1", ec, ex]])

    def await_y0(ec, ex, er):
        landed(y0zone(ec, ex, er), recv_sem.at[RECV["y0", ec, ex, er]])

    def await_y1(rel, ec, ex, er):
        landed(y1zone(rel, ec, ex, er), recv_sem.at[RECV["y1", rel, ec, ex, er]])

    def send_x0(log, rel, ec, ex, h, to, there):
        zone = x0g.at[half_rows(h), xcols(rel, ec, ex)]
        src = zone if rel or ec or ex else x_ref.at[batch(0, 0, 0), half_rows(h)]
        push(log, src, zone, ("x0", there, ec, ex, h), to)

    def send_y0(log, ec, ex):
        zone = y0zone(ec, ex, 0)
        src = zone if ec or ex else y_ref.at[batch(0, 0, 0)]
        push(log, src, zone, ("y0", ec, ex, 1), over_y)

    def send_y1(log, rel, ec, ex, to, there, er):
        zone = y1zone(rel, ec, ex, 0)
        src = zone if rel or ec or ex else y_ref.at[batch(0, 0, 1)]
        push(log, src, zone, ("y1", there, ec, ex, er), to)

    def spread(ec, ex, what, h=0):
        to = dev(y, z, line(ex), core(ec))
        if what == "x0":
            push(sent, x_ref.at[batch(ec, ex, 0), half_rows(h)], x0g.at[half_rows(h), xcols(0, 0, 0)],
                 ("x0", 0, ec, ex, h), to)
        elif what == "y1":
            push(sent, y_ref.at[batch(ec, ex, 1)], y1zone(0, 0, 0, 0), ("y1", 0, ec, ex, 0), to)
        elif what == "x1":
            push(sent, x_ref.at[batch(ec, ex, 1)], xg.at[:, xcols(0, 0, 0)], ("x1", ec, ex), to)
        else:
            push(sent, y_ref.at[batch(ec, ex, 0)], y0zone(0, 0, 0), ("y0", ec, ex, 0), to)

    send_x0(sent, 0, 0, 0, 0, over_half, 1)
    for targets in (((1, 0),), ((0, 1), (1, 1))):
        for h in range(HALVES):
            for ec, ex in targets:
                spread(ec, ex, "x0", h)
        for what in ("y1", "x1", "y0"):
            for ec, ex in targets:
                spread(ec, ex, what)
    def staged(i):
        return xc.at[:, pl.ds(i * depth_x, depth_x)]

    keeps = [
        pltpu.make_async_copy(x_ref.at[batch(0, 0, 1)], xg.at[:, xcols(0, 0, 0)], local_sem.at[0]),
        pltpu.make_async_copy(y_ref.at[batch(0, 0, 0)], y0zone(0, 0, 0), local_sem.at[1]),
        pltpu.make_async_copy(y_ref.at[batch(0, 0, 1)], y1zone(0, 0, 0, 0), local_sem.at[2]),
    ]
    loads = [
        pltpu.make_async_copy(x_ref.at[batch(0, 0, 0), rowsof(i)], staged(i), local_sem.at[4 + i]) for i in range(count)
    ]
    stores = [
        pltpu.make_async_copy(staged(i), x0g.at[rowsof(i), xcols(0, 0, 0)], local_sem.at[4 + count + i])
        for i in range(count)
    ]
    for keep in loads + keeps:
        keep.start()

    def place_own():
        for load, store in zip(loads, stores):
            load.wait()
            store.start()

    def placed_own():
        for store in stores:
            store.wait()

    def dot(a, b):
        return lax.dot_general(a, b, NT, preferred_element_type=jnp.float32).astype(jnp.bfloat16)

    def out0(k):
        slot = lax.rem(k, slots0)
        return remote(og0.at[slot], o_ref.at[x * 2, rowsof(k)], o0_send.at[slot], recv_sem.at[RECV[("out0",)]],
                      dev(y, z, line(1), c))

    def product0(k):
        load = pltpu.make_async_copy(x0g.at[rowsof(k)], xc, local_sem.at[3])
        load.start()
        pl.when(k >= slots0)(lambda: out0(k - slots0).wait_send())
        load.wait()
        og0[lax.rem(k, slots0)] = dot(xc[...], yg0[tile(line(1)), :])
        out0(k).start()
        o_ref[x * 2, rowsof(k)] = dot(xc[...], yg0[tile(x), :])

    TARGETS = ((1, 1), (1, 0), (0, 1))

    def out_part(src, dst, sem, ez, ex):
        kind = "out1" if ez == 0 or ex == 0 else "out2"
        return remote(src, dst, sem, recv_sem.at[RECV[(kind,)]], dev(y, level[ez], line(ex), c))

    def place(ez, ex):
        return tile(line(ex) if ez else lines)

    def out1(r, ez, ex):
        slot = lax.rem(r, slots1)
        return out_part(og1.at[slot, :, place(ez, ex)], o_ref.at[x * 2 + 1, rowsof(r)],
                        o1_send.at[slot * 3 + ez * 2 + ex - 1], ez, ex)

    def free1(r):
        for at in TARGETS:
            out1(r, *at).wait_send()

    def whose(ez, ex):
        return tile(lax.rem(level[ez], 2) * lines + line(ex))

    def near(r, ec, to, sems):
        zone = xg.at[rowsof(r), xpair(0, ec)]
        return remote(zone, zone, near_send.at[r * 2 + ec], sems.at[r * 2 + ec], to)

    def far(r, ec):
        zone = xg.at[rowsof(r), xpair(1, ec)]
        return remote(zone, zone, far_send.at[r * 2 + ec], far_recv.at[r * 2 + ec], over_mid)

    def send_near(r):
        for ec in range(2):
            near(r, ec, over_mid, near_recv).start()

    def far_tail(j, ec):
        at, size = tails[j]
        zone = xg.at[pl.ds(last * chunk + at, size), xpair(1, ec)]
        k = (last + j) * 2 + ec
        return remote(zone, zone, far_send.at[k], far_recv.at[k], over_mid)

    def send_far(r):
        for ec in range(2):
            landed(xg.at[rowsof(r), xpair(1, ec)], up_recv.at[r * 2 + ec])
            far(r, ec).start()

    def send_tails():
        for ec in range(2):
            landed(xg.at[rowsof(last), xpair(1, ec)], up_recv.at[last * 2 + ec])
        for j in range(len(tails)):
            for ec in range(2):
                far_tail(j, ec).start()

    def product1(r):
        for ec in range(2):
            landed(xg.at[rowsof(r), xpair(2, ec)], near_recv.at[r * 2 + ec])
            landed(xg.at[rowsof(r), xpair(3, ec)], far_recv.at[r * 2 + ec])
        pl.when(r >= slots1)(lambda: free1(r - slots1))
        slot = lax.rem(r, slots1)
        og1[slot, :, pl.ds(0, wide)] = dot(xg[rowsof(r), :], yg1[half_cols(lax.rem(partner, 2)), :])
        out1(r, 1, 1).start()
        out1(r, 1, 0).start()
        og1[slot, :, place(0, 1)] = dot(xg[rowsof(r), :], yg1[whose(0, 1), :])
        out1(r, 0, 1).start()
        o_ref[x * 2 + 1, rowsof(r)] = dot(xg[rowsof(r), :], yg1[whose(0, 0), :])

    def out_tail(j, ez, ex):
        at, size = tails[j]
        return out_part(og1.at[last % slots1, pl.ds(at, size), place(ez, ex)],
                        o_ref.at[x * 2 + 1, pl.ds(last * chunk + at, size)],
                        o1_send.at[(slots1 + j) * 3 + ez * 2 + ex - 1], ez, ex)

    def members(ec, far_part):
        third = planes - 1
        if far_part:
            return xpair(3, ec)
        first = jnp.where(level[3] == 0, pair, 0)
        return pl.ds(pl.multiple_of(core(ec) * group + first, pair), third * pair)

    def terms(rows_at, cols_at, far_part):
        total = None
        for ec in range(2):
            at = members(ec, far_part)
            term = lax.dot_general(xg[rows_at, at], yg1[cols_at, at], NT, preferred_element_type=jnp.float32)
            total = term if total is None else total + term
        return total

    def half_cols(q):
        return pl.ds(pl.multiple_of(q * wide, wide), wide)

    def product_last():
        for ec in range(2):
            landed(xg.at[rowsof(last), xpair(2, ec)], near_recv.at[last * 2 + ec])

        def part(q, _):
            acc[:, half_cols(q)] = terms(rowsof(last), half_cols(q), False)
            return 0

        lax.fori_loop(0, 2, part, 0)
        free1(last - slots1)
        for j, (at, size) in enumerate(tails):
            for ec in range(2):
                landed(xg.at[pl.ds(last * chunk + at, size), xpair(3, ec)], far_recv.at[(last + j) * 2 + ec])

            def final(cols_at):
                more = terms(pl.ds(last * chunk + at, size), cols_at, True)
                return (acc[pl.ds(at, size), cols_at] + more).astype(jnp.bfloat16)

            og1[last % slots1, pl.ds(at, size), pl.ds(0, wide)] = final(half_cols(lax.rem(partner, 2)))
            out_tail(j, 1, 1).start()
            out_tail(j, 1, 0).start()
            og1[last % slots1, pl.ds(at, size), place(0, 1)] = final(whose(0, 1))
            out_tail(j, 0, 1).start()
            o_ref[x * 2 + 1, pl.ds(last * chunk + at, size)] = final(whose(0, 0))

    ahead = 4

    @pl.when(inner)
    def _():
        log = list(sent)
        send_x0(log, 0, 0, 0, 0, over_mid, 2)
        send_y1(log, 0, 0, 0, over_y, 0, 1)

        def own_mid(ec, ex, h):
            if ec or ex:
                await_x0(0, ec, ex, h)
            send_x0(log, 0, ec, ex, h, over_mid, 2)

        def own_half(ec, ex, h):
            send_x0(log, 0, ec, ex, h, over_half, 1)

        def outer(ec, ex, h):
            await_x0(1, ec, ex, h)
            send_x0(log, 1, ec, ex, h, over_mid, 3)

        def other(rel, ec, ex, h):
            await_x0(rel, ec, ex, h)
            send_x0(log, rel, ec, ex, h, over_half, rel)

        def side0(ec, ex):
            await_y0(ec, ex, 0)
            send_y0(log, ec, ex)

        def side1(rel, ec, ex):
            await_y1(rel, ec, ex, 0)
            send_y1(log, rel, ec, ex, over_y, rel, 1)

        own_mid(1, 0, 0)
        own_half(1, 0, 0)
        side1(0, 1, 0)
        send_y0(log, 0, 0)
        side0(1, 0)
        place_own()
        for ex_ec in ((0, 1), (1, 1)):
            own_mid(*ex_ec, 0)
            own_half(*ex_ec, 0)
        every = ((0, 0), (1, 0), (0, 1), (1, 1))
        for at in every:
            outer(*at, 0)
            other(2, *at, 0)
        for at in every:
            own_mid(*at, 1)
        other(3, 0, 0, 0)
        outer(0, 0, 1)
        other(3, 1, 0, 0)
        outer(1, 0, 1)
        side1(0, 0, 1)
        other(3, 0, 1, 0)
        outer(0, 1, 1)
        other(3, 1, 1, 0)
        outer(1, 1, 1)
        for at in every:
            own_half(*at, 1)
        side1(0, 1, 1)
        other(2, 0, 0, 1)
        side1(1, 0, 0)
        other(2, 1, 0, 1)
        other(2, 0, 1, 1)
        other(2, 1, 1, 1)
        side1(1, 1, 0)
        keeps[0].wait()
        await_x1(1, 0)
        await_x1(0, 1)
        await_x1(1, 1)
        send_near(0)
        send_near(1)
        other(3, 0, 0, 1)
        other(3, 1, 0, 1)
        side1(1, 0, 1)
        other(3, 0, 1, 1)
        side0(0, 1)
        other(3, 1, 1, 1)
        side1(1, 1, 1)
        side0(1, 1)
        for r in range(ahead):
            send_far(r)
            send_near(r + 2)
        placed_own()
        keeps[1].wait()
        keeps[2].wait()
        for rel in range(2):
            for ec in range(2):
                for ex in range(2):
                    await_y1(rel, ec, ex, 1)

        def both(r, _):
            product1(r)

            @pl.when(r + ahead < last)
            def _():
                send_far(r + ahead)

            @pl.when(r == 0)
            def _():
                send_near(last - 1)

            @pl.when(r == 2)
            def _():
                send_near(last)

            @pl.when(r + ahead == last)
            def _():
                send_tails()

            @pl.when(r == 2)
            def _():
                for ec in range(2):
                    for ex in range(2):
                        await_y0(ec, ex, 1)

            @pl.when((r >= 2) & (r < 6))
            def _():
                def step(k, _):
                    product0((r - 2) * (count // 4) + k)
                    return 0

                lax.fori_loop(0, count // 4, step, 0)

            return 0

        lax.fori_loop(0, last, both, 0)
        product_last()
        for r in range(count):
            for ec in range(2):
                near(r, ec, over_mid, near_recv).wait_send()
                if r < last:
                    far(r, ec).wait_send()
        for j in range(len(tails)):
            for ec in range(2):
                far_tail(j, ec).wait_send()
            for at in TARGETS:
                out_tail(j, *at).wait_send()
        for r in range(count - slots1, last):
            free1(r)
        for k in range(count - slots0, count):
            out0(k).wait_send()
        landed(o_ref.at[line(1) * 2], recv_sem.at[RECV[("out0",)]])
        landed(o_ref.at[line(1) * 2 + 1], recv_sem.at[RECV[("out1",)]])
        for cp in log:
            cp.wait_send()

    @pl.when(jnp.logical_not(inner))
    def _():
        log = list(sent)

        def own(ec, ex, h):
            if ec or ex:
                await_x0(0, ec, ex, h)
            send_x0(log, 0, ec, ex, h, over_half, 1)

        def side0(ec, ex):
            await_y0(ec, ex, 0)
            send_y0(log, ec, ex)

        def down(ec, ex):
            if ec or ex:
                await_y1(0, ec, ex, 0)
            send_y1(log, 0, ec, ex, over_half, 1, 0)

        own(1, 0, 0)
        send_y0(log, 0, 0)
        side0(1, 0)
        place_own()
        own(0, 1, 0)
        own(1, 1, 0)
        for at in ((0, 0), (1, 0), (0, 1), (1, 1)):
            own(*at, 1)
        for at in ((0, 0), (1, 0), (0, 1), (1, 1)):
            down(*at)
        keeps[0].wait()
        await_x1(1, 0)
        await_x1(0, 1)
        await_x1(1, 1)
        for r in range(count):
            for ec in range(2):
                near(r, ec, over_half, up_recv).start()
        side0(0, 1)
        side0(1, 1)
        placed_own()
        keeps[1].wait()
        keeps[2].wait()
        for ec in range(2):
            for ex in range(2):
                await_y0(ec, ex, 1)
        def step(k, _):
            @pl.when(lax.rem(k, count // HALVES) == 0)
            def _():
                for h in range(HALVES):
                    @pl.when(k == h * (count // HALVES))
                    def _():
                        for rel in range(1, 4):
                            for ec in range(2):
                                for ex in range(2):
                                    await_x0(rel, ec, ex, h)

            product0(k)
            return 0

        lax.fori_loop(0, count, step, 0)
        for r in range(count):
            for ec in range(2):
                near(r, ec, over_half, up_recv).wait_send()
        for k in range(count - slots0, count):
            out0(k).wait_send()
        landed(o_ref.at[line(1) * 2], recv_sem.at[RECV[("out0",)]])
        landed(o_ref.at[x * 2 + 1], recv_sem.at[RECV[("out1",)]])
        landed(o_ref.at[line(1) * 2 + 1], recv_sem.at[RECV[("out2",)]])
        for cp in log:
            cp.wait_send()


def routed(sizes, anomaly_x, anomaly_y):
    rows, planes, lines, layers = sizes
    _, height, depth_x = anomaly_x.shape
    width, depth_y = anomaly_y.shape[1:]
    members = depth_y * rows * layers
    count, slots0, slots1 = 8, 4, 4
    chunk = height // count
    dma = pltpu.SemaphoreType.DMA
    any_ = pl.BlockSpec(memory_space=pl.ANY)
    kind = anomaly_x.dtype
    many = dma((2 * count,))
    return pl.pallas_call(
        functools.partial(kernel, sizes),
        out_shape=[
            pltpu.VMEM((planes, height, width), jnp.bfloat16),
            jax.ShapeDtypeStruct((height, members), kind),
        ],
        in_specs=[any_, any_],
        out_specs=[pl.BlockSpec(memory_space=pltpu.VMEM), any_],
        scratch_shapes=[
            pltpu.VMEM((height, members), kind),
            pltpu.VMEM((chunk, members), kind),
            pltpu.VMEM((lines * width, members), kind),
            pltpu.VMEM((2 * lines * width, members), kind),
            pltpu.VMEM((slots0, chunk, width), jnp.bfloat16),
            pltpu.VMEM((slots1, chunk, (lines + 1) * width), jnp.bfloat16),
            pltpu.VMEM((chunk, 2 * lines * width), jnp.float32),
            dma((4 + 2 * count,)), dma((SENDS,)), dma((len(RECV),)),
            many, many, many, dma((2 * count + 6,)), many, dma((2 * count + 6,)),
            dma((slots0,)), dma((3 * slots1 + 12,)),
        ],
        compiler_params=pltpu.CompilerParams(
            collective_id=0, has_side_effects=True, vmem_limit_bytes=54 * 2**20
        ),
    )(anomaly_x, anomaly_y)[0]


def on_device(mesh, anomaly_x, anomaly_y):
    rows, cols, layers = (mesh.shape[name] for name in ("row", "col", "layer"))
    batches, height, depth_x = anomaly_x.shape
    planes = batches // layers
    fits = rows == 2 and layers == 2 and batches == 8 and cols == 2 * planes
    if not fits or depth_x % LANES or height % 128:
        return gathered(anomaly_x, anomaly_y)
    return routed((rows, planes, cols // planes, layers), anomaly_x, anomaly_y)


def solution(mesh):
    placed = (P(None, "row", ("layer", "col")), P(None, "col", ("layer", "row")))
    return jax.shard_map(
        functools.partial(on_device, mesh),
        mesh=mesh, in_specs=placed, out_specs=P("layer", "row", "col"), check_vma=False,
    )
```

```python
import functools

import jax
import jax.numpy as jnp
from jax import lax
from jax.experimental import pallas as pl
from jax.experimental.pallas import tpu as pltpu
from jax.sharding import PartitionSpec as P

LANES = 128
MESH = pl.DeviceIdType.MESH
NT = (((1,), (1,)), ((), ()))


def gathered(anomaly_x, anomaly_y):
    panel_x = lax.all_gather(anomaly_x, "col", axis=2, tiled=True)
    partial_tile = jnp.einsum(
        "bik,bjk->bij",
        panel_x,
        lax.all_gather(anomaly_y, "row", axis=2, tiled=True),
        preferred_element_type=jnp.float32,
    )
    summed = lax.psum_scatter(partial_tile, "layer", scatter_dimension=0, tiled=True)
    return summed.astype(jnp.bfloat16)


HALVES = 2


def plan():
    recv = {}

    def add(*key):
        recv[key] = len(recv)

    for rel in range(4):
        for ec in range(2):
            for ex in range(2):
                for h in range(HALVES):
                    if rel or ec or ex:
                        add("x0", rel, ec, ex, h)
    for ec in range(2):
        for ex in range(2):
            if ec or ex:
                add("x1", ec, ex)
            for yr in range(2):
                if ec or ex or yr:
                    add("y0", ec, ex, yr)
                    add("y1", 0, ec, ex, yr)
                add("y1", 1, ec, ex, yr)
    for kind in ("out0", "out1", "out2"):
        add(kind)
    return recv


RECV = plan()
SENDS = 80


def kernel(
    sizes, x_ref, y_ref, o_ref, x0g, xg, xc, yg0, yg1, og0, og1, acc,
    local_sem, send_sem, recv_sem, up_send, up_recv, near_send, far_send, near_recv, far_recv, o0_send, o1_send,
):
    rows, planes, lines, layers = sizes
    y, col, c = lax.axis_index("row"), lax.axis_index("col"), lax.axis_index("layer")
    z, x = col // lines, lax.rem(col, lines)
    depth_x, depth_y = x_ref.shape[2], y_ref.shape[2]
    height, width = x_ref.shape[1], y_ref.shape[1]
    group = depth_x * planes * lines
    pair = depth_x * lines
    chunk = og0.shape[1]
    count = height // chunk
    slots0, slots1 = og0.shape[0], og1.shape[0]
    last, wide = count - 1, lines * width
    tails = [(j * chunk // 4, chunk // 4) for j in range(4)]

    half = z // 2
    mid, end = 1 + half, 3 * half
    inner = (z == 1) | (z == 2)
    partner = z + 1 - 2 * lax.rem(z, 2)
    across = planes - 1 - z
    level = [z, partner, planes - 1 - mid, planes - 1 - end]

    def core(e):
        return lax.rem(c + e, layers)

    def line(e):
        return lax.rem(x + e, lines)

    def row(e):
        return lax.rem(y + e, rows)

    def dev(yy, zz, xx, cc):
        return {"row": yy, "col": zz * lines + xx, "layer": cc}

    def batch(ec, ex, s):
        return core(ec) * planes + line(ex) * 2 + s

    def xcols(rel, ec, ex):
        return pl.ds(pl.multiple_of(core(ec) * group + (level[rel] * lines + line(ex)) * depth_x, depth_x), depth_x)

    def xpair(rel, ec):
        return pl.ds(pl.multiple_of(core(ec) * group + level[rel] * pair, pair), pair)

    def ycols(ec, er):
        return pl.ds(pl.multiple_of(core(ec) * group + row(er) * depth_y, depth_y), depth_y)

    def y0zone(ec, ex, er):
        return yg0.at[pl.ds(pl.multiple_of(line(ex) * width, width), width), ycols(ec, er)]

    def y1zone(rel, ec, ex, er):
        at = lax.rem(level[rel], 2) * lines * width + line(ex) * width
        return yg1.at[pl.ds(pl.multiple_of(at, width), width), ycols(ec, er)]

    def half_rows(h):
        return pl.ds(h * (height // HALVES), height // HALVES)

    def rowsof(r):
        return pl.ds(pl.multiple_of(r * chunk, chunk), chunk)

    def tile(q):
        return pl.ds(pl.multiple_of(q * width, width), width)

    peers = [dev(y, z, line(ex), core(ec)) for ec in range(2) for ex in range(2) if ec or ex]
    peers += [dev(row(1), z, x, c), dev(y, partner, x, c), dev(y, partner, line(1), c), dev(y, across, x, c)]
    barrier = pltpu.get_barrier_semaphore()
    for peer in peers:
        pl.semaphore_signal(barrier, inc=1, device_id=peer, device_id_type=MESH)
    pl.semaphore_wait(barrier, len(peers))

    over_y, over_half, over_mid = dev(row(1), z, x, c), dev(y, partner, x, c), dev(y, across, x, c)

    def remote(src, dst, s, r, to):
        return pltpu.make_async_remote_copy(
            src_ref=src, dst_ref=dst, send_sem=s, recv_sem=r, device_id=to, device_id_type=MESH
        )

    def landed(dst, sem):
        remote(dst, dst, sem, sem, over_y).wait_recv()

    sent = []

    def push(log, src, dst, key, to):
        cp = remote(src, dst, send_sem.at[len(log)], recv_sem.at[RECV[key]], to)
        cp.start()
        log.append(cp)

    def await_x0(rel, ec, ex, h):
        landed(x0g.at[half_rows(h), xcols(rel, ec, ex)], recv_sem.at[RECV["x0", rel, ec, ex, h]])

    def await_x1(ec, ex):
        landed(xg.at[:, xcols(0, ec, ex)], recv_sem.at[RECV["x1", ec, ex]])

    def await_y0(ec, ex, er):
        landed(y0zone(ec, ex, er), recv_sem.at[RECV["y0", ec, ex, er]])

    def await_y1(rel, ec, ex, er):
        landed(y1zone(rel, ec, ex, er), recv_sem.at[RECV["y1", rel, ec, ex, er]])

    def send_x0(log, rel, ec, ex, h, to, there):
        zone = x0g.at[half_rows(h), xcols(rel, ec, ex)]
        src = zone if rel or ec or ex else x_ref.at[batch(0, 0, 0), half_rows(h)]
        push(log, src, zone, ("x0", there, ec, ex, h), to)

    def send_y0(log, ec, ex):
        zone = y0zone(ec, ex, 0)
        src = zone if ec or ex else y_ref.at[batch(0, 0, 0)]
        push(log, src, zone, ("y0", ec, ex, 1), over_y)

    def send_y1(log, rel, ec, ex, to, there, er):
        zone = y1zone(rel, ec, ex, 0)
        src = zone if rel or ec or ex else y_ref.at[batch(0, 0, 1)]
        push(log, src, zone, ("y1", there, ec, ex, er), to)

    def spread(ec, ex, what, h=0):
        to = dev(y, z, line(ex), core(ec))
        if what == "x0":
            push(sent, x_ref.at[batch(ec, ex, 0), half_rows(h)], x0g.at[half_rows(h), xcols(0, 0, 0)],
                 ("x0", 0, ec, ex, h), to)
        elif what == "y1":
            push(sent, y_ref.at[batch(ec, ex, 1)], y1zone(0, 0, 0, 0), ("y1", 0, ec, ex, 0), to)
        elif what == "x1":
            push(sent, x_ref.at[batch(ec, ex, 1)], xg.at[:, xcols(0, 0, 0)], ("x1", ec, ex), to)
        else:
            push(sent, y_ref.at[batch(ec, ex, 0)], y0zone(0, 0, 0), ("y0", ec, ex, 0), to)

    send_x0(sent, 0, 0, 0, 0, over_half, 1)
    for targets in (((1, 0),), ((0, 1), (1, 1))):
        for h in range(HALVES):
            for ec, ex in targets:
                spread(ec, ex, "x0", h)
        for what in ("y1", "x1", "y0"):
            for ec, ex in targets:
                spread(ec, ex, what)
    def staged(i):
        return xc.at[:, pl.ds(i * depth_x, depth_x)]

    keeps = [
        pltpu.make_async_copy(x_ref.at[batch(0, 0, 1)], xg.at[:, xcols(0, 0, 0)], local_sem.at[0]),
        pltpu.make_async_copy(y_ref.at[batch(0, 0, 0)], y0zone(0, 0, 0), local_sem.at[1]),
        pltpu.make_async_copy(y_ref.at[batch(0, 0, 1)], y1zone(0, 0, 0, 0), local_sem.at[2]),
    ]
    loads = [
        pltpu.make_async_copy(x_ref.at[batch(0, 0, 0), rowsof(i)], staged(i), local_sem.at[4 + i]) for i in range(count)
    ]
    stores = [
        pltpu.make_async_copy(staged(i), x0g.at[rowsof(i), xcols(0, 0, 0)], local_sem.at[4 + count + i])
        for i in range(count)
    ]
    for keep in loads + keeps:
        keep.start()

    def place_own():
        for load, store in zip(loads, stores):
            load.wait()
            store.start()

    def placed_own():
        for store in stores:
            store.wait()

    def dot(a, b):
        return lax.dot_general(a, b, NT, preferred_element_type=jnp.float32).astype(jnp.bfloat16)

    def out0(k):
        slot = lax.rem(k, slots0)
        return remote(og0.at[slot], o_ref.at[x * 2, rowsof(k)], o0_send.at[slot], recv_sem.at[RECV[("out0",)]],
                      dev(y, z, line(1), c))

    def product0(k):
        load = pltpu.make_async_copy(x0g.at[rowsof(k)], xc, local_sem.at[3])
        load.start()
        pl.when(k >= slots0)(lambda: out0(k - slots0).wait_send())
        load.wait()
        og0[lax.rem(k, slots0)] = dot(xc[...], yg0[tile(line(1)), :])
        out0(k).start()
        o_ref[x * 2, rowsof(k)] = dot(xc[...], yg0[tile(x), :])

    TARGETS = ((1, 1), (1, 0), (0, 1))

    def out_part(src, dst, sem, ez, ex):
        kind = "out1" if ez == 0 or ex == 0 else "out2"
        return remote(src, dst, sem, recv_sem.at[RECV[(kind,)]], dev(y, level[ez], line(ex), c))

    def place(ez, ex):
        return tile(line(ex) if ez else lines)

    def out1(r, ez, ex):
        slot = lax.rem(r, slots1)
        return out_part(og1.at[slot, :, place(ez, ex)], o_ref.at[x * 2 + 1, rowsof(r)],
                        o1_send.at[slot * 3 + ez * 2 + ex - 1], ez, ex)

    def free1(r):
        for at in TARGETS:
            out1(r, *at).wait_send()

    def whose(ez, ex):
        return tile(lax.rem(level[ez], 2) * lines + line(ex))

    def near(r, ec, to, sems):
        zone = xg.at[rowsof(r), xpair(0, ec)]
        return remote(zone, zone, near_send.at[r * 2 + ec], sems.at[r * 2 + ec], to)

    def far(r, ec):
        zone = xg.at[rowsof(r), xpair(1, ec)]
        return remote(zone, zone, far_send.at[r * 2 + ec], far_recv.at[r * 2 + ec], over_mid)

    def send_near(r):
        for ec in range(2):
            near(r, ec, over_mid, near_recv).start()

    def far_tail(j, ec):
        at, size = tails[j]
        zone = xg.at[pl.ds(last * chunk + at, size), xpair(1, ec)]
        k = (last + j) * 2 + ec
        return remote(zone, zone, far_send.at[k], far_recv.at[k], over_mid)

    def send_far(r):
        for ec in range(2):
            landed(xg.at[rowsof(r), xpair(1, ec)], up_recv.at[r * 2 + ec])
            far(r, ec).start()

    def send_tails():
        for ec in range(2):
            landed(xg.at[rowsof(last), xpair(1, ec)], up_recv.at[last * 2 + ec])
        for j in range(len(tails)):
            for ec in range(2):
                far_tail(j, ec).start()

    def product1(r):
        for ec in range(2):
            landed(xg.at[rowsof(r), xpair(2, ec)], near_recv.at[r * 2 + ec])
            landed(xg.at[rowsof(r), xpair(3, ec)], far_recv.at[r * 2 + ec])
        pl.when(r >= slots1)(lambda: free1(r - slots1))
        slot = lax.rem(r, slots1)
        og1[slot, :, pl.ds(0, wide)] = dot(xg[rowsof(r), :], yg1[half_cols(lax.rem(partner, 2)), :])
        out1(r, 1, 1).start()
        out1(r, 1, 0).start()
        og1[slot, :, place(0, 1)] = dot(xg[rowsof(r), :], yg1[whose(0, 1), :])
        out1(r, 0, 1).start()
        o_ref[x * 2 + 1, rowsof(r)] = dot(xg[rowsof(r), :], yg1[whose(0, 0), :])

    def out_tail(j, ez, ex):
        at, size = tails[j]
        return out_part(og1.at[last % slots1, pl.ds(at, size), place(ez, ex)],
                        o_ref.at[x * 2 + 1, pl.ds(last * chunk + at, size)],
                        o1_send.at[(slots1 + j) * 3 + ez * 2 + ex - 1], ez, ex)

    def members(ec, far_part):
        third = planes - 1
        if far_part:
            return xpair(3, ec)
        first = jnp.where(level[3] == 0, pair, 0)
        return pl.ds(pl.multiple_of(core(ec) * group + first, pair), third * pair)

    def terms(rows_at, cols_at, far_part):
        total = None
        for ec in range(2):
            at = members(ec, far_part)
            term = lax.dot_general(xg[rows_at, at], yg1[cols_at, at], NT, preferred_element_type=jnp.float32)
            total = term if total is None else total + term
        return total

    def half_cols(q):
        return pl.ds(pl.multiple_of(q * wide, wide), wide)

    def product_last():
        for ec in range(2):
            landed(xg.at[rowsof(last), xpair(2, ec)], near_recv.at[last * 2 + ec])

        def part(q, _):
            acc[:, half_cols(q)] = terms(rowsof(last), half_cols(q), False)
            return 0

        lax.fori_loop(0, 2, part, 0)
        free1(last - slots1)
        for j, (at, size) in enumerate(tails):
            for ec in range(2):
                landed(xg.at[pl.ds(last * chunk + at, size), xpair(3, ec)], far_recv.at[(last + j) * 2 + ec])

            def final(cols_at):
                more = terms(pl.ds(last * chunk + at, size), cols_at, True)
                return (acc[pl.ds(at, size), cols_at] + more).astype(jnp.bfloat16)

            for ex in (1, 0):
                og1[last % slots1, pl.ds(at, size), place(1, ex)] = final(whose(1, ex))
                out_tail(j, 1, ex).start()
            og1[last % slots1, pl.ds(at, size), place(0, 1)] = final(whose(0, 1))
            out_tail(j, 0, 1).start()
            o_ref[x * 2 + 1, pl.ds(last * chunk + at, size)] = final(whose(0, 0))

    ahead = 4

    @pl.when(inner)
    def _():
        log = list(sent)
        send_x0(log, 0, 0, 0, 0, over_mid, 2)
        send_y1(log, 0, 0, 0, over_y, 0, 1)

        def own_mid(ec, ex, h):
            if ec or ex:
                await_x0(0, ec, ex, h)
            send_x0(log, 0, ec, ex, h, over_mid, 2)

        def own_half(ec, ex, h):
            send_x0(log, 0, ec, ex, h, over_half, 1)

        def outer(ec, ex, h):
            await_x0(1, ec, ex, h)
            send_x0(log, 1, ec, ex, h, over_mid, 3)

        def other(rel, ec, ex, h):
            await_x0(rel, ec, ex, h)
            send_x0(log, rel, ec, ex, h, over_half, rel)

        def side0(ec, ex):
            await_y0(ec, ex, 0)
            send_y0(log, ec, ex)

        def side1(rel, ec, ex):
            await_y1(rel, ec, ex, 0)
            send_y1(log, rel, ec, ex, over_y, rel, 1)

        own_mid(1, 0, 0)
        own_half(1, 0, 0)
        side1(0, 1, 0)
        send_y0(log, 0, 0)
        side0(1, 0)
        place_own()
        for ex_ec in ((0, 1), (1, 1)):
            own_mid(*ex_ec, 0)
            own_half(*ex_ec, 0)
        every = ((0, 0), (1, 0), (0, 1), (1, 1))
        for at in every:
            outer(*at, 0)
            other(2, *at, 0)
        for at in every:
            own_mid(*at, 1)
        other(3, 0, 0, 0)
        outer(0, 0, 1)
        other(3, 1, 0, 0)
        outer(1, 0, 1)
        side1(0, 0, 1)
        other(3, 0, 1, 0)
        outer(0, 1, 1)
        other(3, 1, 1, 0)
        outer(1, 1, 1)
        for at in every:
            own_half(*at, 1)
        side1(0, 1, 1)
        other(2, 0, 0, 1)
        side1(1, 0, 0)
        other(2, 1, 0, 1)
        other(2, 0, 1, 1)
        other(2, 1, 1, 1)
        side1(1, 1, 0)
        keeps[0].wait()
        await_x1(1, 0)
        await_x1(0, 1)
        await_x1(1, 1)
        send_near(0)
        send_near(1)
        other(3, 0, 0, 1)
        other(3, 1, 0, 1)
        side1(1, 0, 1)
        other(3, 0, 1, 1)
        side0(0, 1)
        other(3, 1, 1, 1)
        side1(1, 1, 1)
        side0(1, 1)
        for r in range(ahead):
            send_far(r)
            send_near(r + 2)
        placed_own()
        keeps[1].wait()
        keeps[2].wait()
        for rel in range(2):
            for ec in range(2):
                for ex in range(2):
                    await_y1(rel, ec, ex, 1)

        def both(r, _):
            product1(r)

            @pl.when(r + ahead < last)
            def _():
                send_far(r + ahead)

            @pl.when(r == 0)
            def _():
                send_near(last - 1)

            @pl.when(r == 2)
            def _():
                send_near(last)

            @pl.when(r + ahead == last)
            def _():
                send_tails()

            @pl.when(r == 2)
            def _():
                for ec in range(2):
                    for ex in range(2):
                        await_y0(ec, ex, 1)

            @pl.when((r >= 2) & (r < 6))
            def _():
                def step(k, _):
                    product0((r - 2) * (count // 4) + k)
                    return 0

                lax.fori_loop(0, count // 4, step, 0)

            return 0

        lax.fori_loop(0, last, both, 0)
        for cp in log:
            cp.wait_send()
        product_last()
        for r in range(count):
            for ec in range(2):
                near(r, ec, over_mid, near_recv).wait_send()
                if r < last:
                    far(r, ec).wait_send()
        for j in range(len(tails)):
            for ec in range(2):
                far_tail(j, ec).wait_send()
            for at in TARGETS:
                out_tail(j, *at).wait_send()
        for r in range(count - slots1, last):
            free1(r)
        for k in range(count - slots0, count):
            out0(k).wait_send()
        landed(o_ref.at[line(1) * 2], recv_sem.at[RECV[("out0",)]])
        landed(o_ref.at[line(1) * 2 + 1], recv_sem.at[RECV[("out1",)]])

    @pl.when(jnp.logical_not(inner))
    def _():
        log = list(sent)

        def own(ec, ex, h):
            if ec or ex:
                await_x0(0, ec, ex, h)
            send_x0(log, 0, ec, ex, h, over_half, 1)

        def side0(ec, ex):
            await_y0(ec, ex, 0)
            send_y0(log, ec, ex)

        def down(ec, ex):
            if ec or ex:
                await_y1(0, ec, ex, 0)
            send_y1(log, 0, ec, ex, over_half, 1, 0)

        own(1, 0, 0)
        send_y0(log, 0, 0)
        side0(1, 0)
        place_own()
        own(0, 1, 0)
        own(1, 1, 0)
        for at in ((0, 0), (1, 0), (0, 1), (1, 1)):
            own(*at, 1)
        for at in ((0, 0), (1, 0), (0, 1), (1, 1)):
            down(*at)
        keeps[0].wait()
        await_x1(1, 0)
        await_x1(0, 1)
        await_x1(1, 1)
        for r in range(count):
            for ec in range(2):
                near(r, ec, over_half, up_recv).start()
        side0(0, 1)
        side0(1, 1)
        placed_own()
        keeps[1].wait()
        keeps[2].wait()
        for ec in range(2):
            for ex in range(2):
                await_y0(ec, ex, 1)
        def step(k, _):
            @pl.when(lax.rem(k, count // HALVES) == 0)
            def _():
                for h in range(HALVES):
                    @pl.when(k == h * (count // HALVES))
                    def _():
                        for rel in range(1, 4):
                            for ec in range(2):
                                for ex in range(2):
                                    await_x0(rel, ec, ex, h)

            product0(k)
            return 0

        lax.fori_loop(0, count, step, 0)
        for r in range(count):
            for ec in range(2):
                near(r, ec, over_half, up_recv).wait_send()
        for k in range(count - slots0, count):
            out0(k).wait_send()
        for cp in log:
            cp.wait_send()
        landed(o_ref.at[line(1) * 2], recv_sem.at[RECV[("out0",)]])
        landed(o_ref.at[x * 2 + 1], recv_sem.at[RECV[("out1",)]])
        landed(o_ref.at[line(1) * 2 + 1], recv_sem.at[RECV[("out2",)]])


def routed(sizes, anomaly_x, anomaly_y):
    rows, planes, lines, layers = sizes
    _, height, depth_x = anomaly_x.shape
    width, depth_y = anomaly_y.shape[1:]
    members = depth_y * rows * layers
    count, slots0, slots1 = 8, 4, 4
    chunk = height // count
    dma = pltpu.SemaphoreType.DMA
    any_ = pl.BlockSpec(memory_space=pl.ANY)
    kind = anomaly_x.dtype
    many = dma((2 * count,))
    return pl.pallas_call(
        functools.partial(kernel, sizes),
        out_shape=[
            pltpu.VMEM((planes, height, width), jnp.bfloat16),
            jax.ShapeDtypeStruct((height, members), kind),
        ],
        in_specs=[any_, any_],
        out_specs=[pl.BlockSpec(memory_space=pltpu.VMEM), any_],
        scratch_shapes=[
            pltpu.VMEM((height, members), kind),
            pltpu.VMEM((chunk, members), kind),
            pltpu.VMEM((lines * width, members), kind),
            pltpu.VMEM((2 * lines * width, members), kind),
            pltpu.VMEM((slots0, chunk, width), jnp.bfloat16),
            pltpu.VMEM((slots1, chunk, (lines + 1) * width), jnp.bfloat16),
            pltpu.VMEM((chunk, 2 * lines * width), jnp.float32),
            dma((4 + 2 * count,)), dma((SENDS,)), dma((len(RECV),)),
            many, many, many, dma((2 * count + 6,)), many, dma((2 * count + 6,)),
            dma((slots0,)), dma((3 * slots1 + 12,)),
        ],
        compiler_params=pltpu.CompilerParams(
            collective_id=0, has_side_effects=True, vmem_limit_bytes=54 * 2**20
        ),
    )(anomaly_x, anomaly_y)[0]


def on_device(mesh, anomaly_x, anomaly_y):
    rows, cols, layers = (mesh.shape[name] for name in ("row", "col", "layer"))
    batches, height, depth_x = anomaly_x.shape
    planes = batches // layers
    fits = rows == 2 and layers == 2 and batches == 8 and cols == 2 * planes
    if not fits or depth_x % LANES or height % 128:
        return gathered(anomaly_x, anomaly_y)
    return routed((rows, planes, cols // planes, layers), anomaly_x, anomaly_y)


def solution(mesh):
    placed = (P(None, "row", ("layer", "col")), P(None, "col", ("layer", "row")))
    return jax.shard_map(
        functools.partial(on_device, mesh),
        mesh=mesh, in_specs=placed, out_specs=P("layer", "row", "col"), check_vma=False,
    )
```
